32 devices in a mesh: gx: 8 (over z, x), gy: 4 (over y, core).
Axes of the slice: x: 2, y: 2, z: 4, core: 2. Of those that a mesh axis runs over, the one named last changes fastest.
Arguments:
- volume: bfloat16 [16, 32, 32, 256], P(None, 'gx', 'gy'), may hold values from -6 to 6
- fine_kernel: bfloat16 [3, 3, 3, 16, 16], replicated, may hold values from -0.3125 to 0.3125
- coarse_kernel: bfloat16 [3, 3, 3, 32, 16], replicated, may hold values from -0.3125 to 0.3125
- fine_cotangent: bfloat16 [16, 32, 32, 256], P(None, 'gx', 'gy'), may hold values from -6 to 6
- coarse_cotangent: bfloat16 [32, 16, 16, 128], P(None, 'gx', 'gy'), may hold values from -18 to 18
Outputs:
- fine_out: bfloat16 [16, 32, 32, 256], P(None, 'gx', 'gy')
- coarse_out: bfloat16 [32, 16, 16, 128], P(None, 'gx', 'gy')
- volume_grad: bfloat16 [16, 32, 32, 256], P(None, 'gx', 'gy')
- fine_kernel_grad: float32 [3, 3, 3, 16, 16], replicated
- coarse_kernel_grad: float32 [3, 3, 3, 32, 16], replicated
The draws below stay inside these ranges and needn't reach their ends.
All inputs are finite; a program needn't handle non-finite values.
Results may differ from the reference program's by a relative error of at most 0.0064.
Values may be sent and summed in bfloat16 or wider, within the bound.
No kernel may reach another device: no remote copies, remote signals or barrier semaphores. Data moves between devices by JAX's collectives and lax.ppermute only.
A program may use at most 64 MiB of HBM per device.

```python
import jax
import jax.numpy as jnp
from jax import lax

C1 = 16
C2 = 32
NZ = 32
NY = 32
NX = 256


def steps_of(key, extent, pieces, low, high):
    gain, own = 1.0, jax.random.fold_in(key, 6)
    for axis_at, shards_of in pieces:
        steps = jnp.exp(jax.random.uniform(jax.random.fold_in(own, axis_at), (shards_of,), jnp.float32, low / len(pieces), high / len(pieces)))
        gain = gain * jnp.repeat(steps, extent[axis_at] // shards_of).reshape([-1 if axis == axis_at else 1 for axis in range(len(extent))])
    return gain


def centred(own_key, extent, width, bound, split=(), kind=jnp.bfloat16):
    entries = jax.random.normal(own_key, extent, jnp.float32) * width
    if len(split) > 0:
        entries = steps_of(own_key, extent, split, -0.22, 0.18) * entries
    return jnp.clip(entries, min=-bound, max=bound).astype(kind)


def setup_inputs(seed: int = 0) -> dict:
    seeds = jax.random.split(jax.random.key(seed), 6)
    return {
        "volume": centred(seeds[0], (C1, NZ, NY, NX), 1.0, 6.0, ((1, 8), (2, 4))),
        "fine_kernel": centred(seeds[1], (3, 3, 3, C1, C1), (27 * C1) ** -0.5, 0.3125),
        "coarse_kernel": centred(seeds[2], (3, 3, 3, C2, C1), (27 * C1) ** -0.5, 0.3125),
        "fine_cotangent": centred(seeds[3], (C1, NZ, NY, NX), 1.0, 6.0, ((1, 8), (2, 4))),
        "coarse_cotangent": centred(seeds[4], (C2, NZ // 2, NY // 2, NX // 2), 3.0, 18.0, ((1, 8), (2, 4))),
    }


def silu_slope(values):
    sigma = jax.nn.sigmoid(values)
    return sigma * (1.0 + values * (1.0 - sigma))


def pad_cells(values):
    return jnp.pad(values, ((0, 0), (1, 1), (1, 1), (1, 1)))


def correlate(padded, weights, flipped, depth_cells, row_count, width_cells):
    summed = None
    for shift_z in range(3):
        for shift_y in range(3):
            for shift_x in range(3):
                if flipped:
                    matrix = weights[shift_z, shift_y, shift_x].T
                    start_z, start_y, start_x = 2 - shift_z, 2 - shift_y, 2 - shift_x
                else:
                    matrix = weights[shift_z, shift_y, shift_x]
                    start_z, start_y, start_x = shift_z, shift_y, shift_x
                piece = padded[:, start_z:start_z + depth_cells, start_y:start_y + row_count, start_x:start_x + width_cells]
                piece = piece.reshape(padded.shape[0], -1)
                contrib = jnp.dot(matrix, piece, preferred_element_type=jnp.float32)
                summed = contrib if summed is None else summed + contrib
    return summed.reshape(-1, depth_cells, row_count, width_cells)


def kernel_terms(slope, padded):
    depth_cells, row_count, width_cells = slope.shape[1:]
    flat_slope = slope.reshape(slope.shape[0], -1)
    stacked = []
    for shift_z in range(3):
        for shift_y in range(3):
            for shift_x in range(3):
                piece = padded[:, shift_z:shift_z + depth_cells, shift_y:shift_y + row_count, shift_x:shift_x + width_cells]
                piece = piece.reshape(padded.shape[0], -1)
                stacked.append(lax.dot_general(flat_slope, piece, (((1,), (1,)), ((), ())), preferred_element_type=jnp.float32))
    return jnp.stack(stacked).reshape(3, 3, 3, slope.shape[0], padded.shape[0])


def pool_mean(values):
    chans, depth_cells, row_count, width_cells = values.shape
    blocks = values.astype(jnp.float32).reshape(chans, depth_cells // 2, 2, row_count // 2, 2, width_cells // 2, 2)
    return blocks.mean(axis=(2, 4, 6))


def spread_cells(grads):
    chans, depth_cells, row_count, width_cells = grads.shape
    wide = jnp.broadcast_to(grads[:, :, None, :, None, :, None], (chans, depth_cells, 2, row_count, 2, width_cells, 2))
    return wide.reshape(chans, 2 * depth_cells, 2 * row_count, 2 * width_cells) / 8.0


def reference(volume, fine_kernel, coarse_kernel, fine_cotangent, coarse_cotangent):
    fine_shape = volume.shape[1:]
    padded = pad_cells(volume)
    fine_pre = correlate(padded, fine_kernel, False, *fine_shape)
    fine_out = (volume.astype(jnp.float32) + jax.nn.silu(fine_pre)).astype(jnp.bfloat16)
    pooled = pool_mean(fine_out).astype(jnp.bfloat16)
    coarse_shape = pooled.shape[1:]
    pooled_pad = pad_cells(pooled)
    coarse_pre = correlate(pooled_pad, coarse_kernel, False, *coarse_shape)
    coarse_out = jax.nn.silu(coarse_pre).astype(jnp.bfloat16)
    coarse_slope = (coarse_cotangent.astype(jnp.float32) * silu_slope(coarse_pre)).astype(jnp.bfloat16)
    pooled_grad = correlate(pad_cells(coarse_slope), coarse_kernel, True, *coarse_shape)
    fine_grad = fine_cotangent.astype(jnp.float32) + spread_cells(pooled_grad)
    fine_slope = (fine_grad * silu_slope(fine_pre)).astype(jnp.bfloat16)
    volume_grad = (fine_grad + correlate(pad_cells(fine_slope), fine_kernel, True, *fine_shape)).astype(jnp.bfloat16)
    fine_kernel_grad = kernel_terms(fine_slope, padded) * (NZ * NY * NX) ** -0.5
    coarse_kernel_grad = kernel_terms(coarse_slope, pooled_pad) * (NZ * NY * NX // 8) ** -0.5
    return fine_out, coarse_out, volume_grad, fine_kernel_grad, coarse_kernel_grad
```

```python
import functools

import jax
import jax.numpy as jnp
from jax import lax
from jax.experimental import pallas as pl
from jax.experimental.pallas import tpu as pltpu
from jax.sharding import PartitionSpec as P

F32 = jnp.float32
BF16 = jnp.bfloat16


def mm(left, right):
    return jnp.dot(left, right, preferred_element_type=F32)


def mm_t(left, right):
    return lax.dot_general(left, right, (((1,), (1,)), ((), ())), preferred_element_type=F32)


def one_hot(shape, rule):
    rows = lax.broadcasted_iota(jnp.int32, shape, 0)
    cols = lax.broadcasted_iota(jnp.int32, shape, 1)
    return jnp.where(rule(rows, cols), 1.0, 0.0).astype(BF16)


def swap_matrix(outer, inner):
    count = outer * inner
    return one_hot((count, count), lambda r, c: c == (r % inner) * outer + r // inner)


def moved(values, width, offset):
    lanes = values.shape[1]
    place = lax.broadcasted_iota(jnp.int32, values.shape, 1) % width
    if offset == 1:
        return jnp.where(place == 0, 0.0, pltpu.roll(values, 1, 1))
    return jnp.where(place == width - 1, 0.0, pltpu.roll(values, lanes - 1, 1))


def combine(parts, width):
    rows = parts.shape[0] // 3
    return (
        parts[rows : 2 * rows]
        + moved(parts[:rows], width, 1)
        + moved(parts[2 * rows :], width, -1)
    )


def to_rows(values):
    chans, rows, width = values.shape
    return values.astype(F32).reshape(chans * rows, width).astype(BF16)


def band(taps_ref, out_ref, out_chans, in_chans, out_rows):
    wide = (out_rows + 2) * in_chans
    spread = one_hot((in_chans, wide), lambda r, c: c % in_chans == r)
    tiled = mm(taps_ref[...], spread)
    block = lax.broadcasted_iota(jnp.int32, (out_chans, wide), 1) // in_chans
    for a in range(3):
        for c in range(3):
            taps = [
                tiled[((a * 3 + b) * 3 + c) * out_chans : ((a * 3 + b) * 3 + c + 1) * out_chans]
                for b in range(3)
            ]
            for y in range(out_rows):
                value = jnp.where(
                    block == y,
                    taps[0],
                    jnp.where(block == y + 1, taps[1], jnp.where(block == y + 2, taps[2], 0.0)),
                )
                start = (c * out_rows + y) * out_chans
                out_ref[a, start : start + out_chans, :] = value.astype(BF16)


def weights_kernel(kf, kft, kc, kct, wa, wt, wc, wct, *, c1, c2, ny):
    band(kf, wa, c1, c1, ny + 2)
    band(kft, wt, c1, c1, ny)
    band(kc, wc, c2, c1, ny // 2 + 4)
    band(kct, wct, c1, c2, ny // 2 + 2)


def cot_pack_kernel(fc, cc, dn, up):
    c1, nz = fc.shape[:2]
    c2 = cc.shape[0]
    dn[:c1] = fc[:, 0]
    up[:c1] = fc[:, nz - 1]
    for ref in (dn, up):
        ref[c1:, :, : cc.shape[2]] = cc[: c2 // 2]
        ref[c1:, :, cc.shape[2] :] = cc[c2 // 2 :]


def rows_kernel(vol, lo, hi, own, dn, up):
    chans, nz, ny, nx = vol.shape
    swap = swap_matrix(ny, chans)
    depth = lo.shape[1]
    layers = [(lo, z) for z in range(depth)] + [(vol, z) for z in range(nz)]
    layers += [(hi, z) for z in range(depth)]
    edge = 2 * chans
    for place, (ref, z) in enumerate(layers):
        value = mm(swap, to_rows(ref[:, z])).astype(BF16)
        span = slice(place * nx, (place + 1) * nx)
        own[:, span] = value
        dn[:, span] = value[:edge]
        up[:, span] = value[-edge:]


def fine_kernel_fn(flags, xo, xl, xh, wa, fo_out, sl_out, pz_dn, pz_up, pz_own, *, c1, nz, ny, nx):
    swap_back = swap_matrix(c1, ny)
    pool = one_hot((nx, nx // 2), lambda r, c: r // 2 == c)
    sums = None
    half = nx // 2
    for layer in range(nz + 4):
        parts = None
        for dz in range(3):
            span = slice((layer + dz) * nx, (layer + dz + 1) * nx)
            x = jnp.concatenate([xl[:, span], xo[:, span], xh[:, span]], axis=0)
            term = mm(wa[dz], x)
            parts = term if parts is None else parts + term
        pre = combine(parts, nx)
        sig = jax.nn.sigmoid(pre)
        span = slice((layer + 1) * nx, (layer + 2) * nx)
        inner = slice(c1, c1 + c1 * ny)
        fo = (xo[:, span].astype(F32) + pre[inner] * sig[inner]).astype(BF16)
        if 1 <= layer <= nz + 2:
            sl_out[:, (layer - 1) * nx : layer * nx] = sig * (1.0 + pre * (1.0 - sig))
        if 2 <= layer < nz + 2:
            fo_out[:, layer - 2] = mm(swap_back, fo).reshape(c1, ny, nx).astype(BF16)
        pooled = mm(fo, pool)
        if layer % 2 == 0:
            sums = pooled
            continue
        sums = sums + pooled
        rows = [
            sums[2 * r * c1 : (2 * r + 1) * c1] + sums[(2 * r + 1) * c1 : (2 * r + 2) * c1]
            for r in range(ny // 2)
        ]
        value = jnp.concatenate(rows, axis=0) * 0.125
        place = layer // 2
        last = nz // 2 + 1
        if place == 0:
            value = jnp.where(flags[0] != 0, 0.0, value)
        if place == last:
            value = jnp.where(flags[1] != 0, 0.0, value)
        value = value.astype(BF16)
        if place < last:
            pz_up[:, place * half : (place + 1) * half] = value
        if place > 0:
            pz_dn[:, (place - 1) * half : place * half] = value
        if 0 < place < last:
            pz_own[:, (place - 1) * half : place * half] = value


def cot_rows_kernel(fc, cc, lo, hi, fc_out, cc_out, dn, up, *, c1, c2, ny):
    nz, nx = fc.shape[1], fc.shape[3]
    half = nx // 2
    hz, hy = nz // 2, ny // 2
    swap = swap_matrix(ny, c1)
    layers = [lo[:c1]] + [fc[:, z] for z in range(nz)] + [hi[:c1]]
    for place, value in enumerate(layers):
        span = slice(place * nx, (place + 1) * nx)
        fc_out[:, span] = mm(swap, to_rows(value)).astype(BF16)
    swap_c = swap_matrix(hz * hy, c2)
    blocks = [
        jnp.concatenate([lo[c1:, :, :half], lo[c1:, :, half:]], axis=0),
        cc[...],
        jnp.concatenate([hi[c1:, :, :half], hi[c1:, :, half:]], axis=0),
    ]
    for index, block in enumerate(blocks):
        value = mm(swap_c, to_rows(block)).astype(BF16)
        for z in range(hz):
            place = index * hz + z
            cc_out[:, place * half : (place + 1) * half] = value[z * hy * c2 : (z + 1) * hy * c2]
    wide = cc_out.shape[1]
    edge = 2 * c2
    for ref, fine_rows, coarse_rows in (
        (dn, slice(0, c1), slice(0, edge)),
        (up, slice((ny - 1) * c1, ny * c1), slice((hy - 2) * c2, hy * c2)),
    ):
        ref[:edge] = cc_out[coarse_rows]
        ref[edge : edge + c1] = fc_out[fine_rows, :wide]
        ref[edge + c1 : edge + 2 * c1] = fc_out[fine_rows, wide:]


def pooled_rows_kernel(lo, own, hi, dn, up):
    edge = dn.shape[0]
    start = 0
    for ref in (lo, own, hi):
        width = ref.shape[1]
        dn[:, start : start + width] = ref[:edge]
        up[:, start : start + width] = ref[-edge:]
        start += width


def coarse_kernel_fn(
    flags, po, pzl, pzh, pyl, pyh, cc, fc, cyl, cyh, sl, xo, xl, xh, wc, wct,
    co_out, fs_out, fg_out, g_out, p_ref, cs_ref, *, c1, c2, nz, ny, nx,
):
    half, hz, hy = nx // 2, nz // 2, ny // 2
    three = 3 * c1
    p_ref[:three] = pyl[...]
    p_ref[three + hy * c1 :] = pyh[...]
    start = 0
    for ref in (pzl, po, pzh):
        p_ref[three : three + hy * c1, start : start + ref.shape[1]] = ref[...]
        start += ref.shape[1]
    edge = 2 * c2
    swap_c = swap_matrix(c2, hz * hy)
    for pair in range((hz + 4) // 2):
        parts = None
        for dz in range(3):
            first = (2 * pair + dz) * half
            term = mm(wc[dz], p_ref[:, first : first + nx])
            parts = term if parts is None else parts + term
        pre = combine(parts, half)
        sig = jax.nn.sigmoid(pre)
        span = slice(pair * nx, (pair + 1) * nx)
        cot = jnp.concatenate([cyl[:edge, span], cc[:, span], cyh[:edge, span]], axis=0)
        cs_ref[:, span] = (cot.astype(F32) * (sig * (1.0 + pre * (1.0 - sig)))).astype(BF16)
        if pair == 1:
            inner = slice(edge, edge + hy * c2)
            out = (pre[inner] * sig[inner]).astype(BF16)
            stacked = jnp.concatenate([out[:, :half], out[:, half:]], axis=0)
            co_out[...] = mm(swap_c, stacked).astype(BF16)
    widen = one_hot((half, nx), lambda r, c: c // 2 == r)
    wide = cc.shape[1]
    for pair in range((hz + 2) // 2):
        parts = None
        for dz in range(3):
            first = (2 * pair + dz) * half
            term = mm(wct[dz], cs_ref[:, first : first + nx])
            parts = term if parts is None else parts + term
        grad = combine(parts, half) * 0.125
        high = grad.astype(BF16)
        low = (grad - high.astype(F32)).astype(BF16)
        for side in range(2):
            lanes = slice(side * half, (side + 1) * half)
            up = mm(high[:, lanes], widen) + mm(low[:, lanes], widen)
            blocks = [up[(y + 2) // 2 * c1 : (y + 2) // 2 * c1 + c1] for y in range(-1, ny + 1)]
            spread = jnp.concatenate(blocks, axis=0)
            coarse_layer = 2 * pair + side - 1
            for layer in (2 * coarse_layer, 2 * coarse_layer + 1):
                if not -1 <= layer <= nz:
                    continue
                place = layer + 1
                span = slice(place * nx, (place + 1) * nx)
                fold = place * nx // wide
                inside = slice(place * nx - fold * wide, (place + 1) * nx - fold * wide)
                edge_rows = slice(edge + fold * c1, edge + (fold + 1) * c1)
                cot = jnp.concatenate(
                    [cyl[edge_rows, inside], fc[:, span], cyh[edge_rows, inside]], axis=0
                )
                total = cot.astype(F32) + spread
                slope = total * sl[:, span]
                row = lax.broadcasted_iota(jnp.int32, slope.shape, 0) // c1
                outside = jnp.logical_and(row == 0, flags[2] != 0)
                outside = jnp.logical_or(outside, jnp.logical_and(row == ny + 1, flags[3] != 0))
                if layer == -1:
                    outside = jnp.logical_or(outside, flags[0] != 0)
                if layer == nz:
                    outside = jnp.logical_or(outside, flags[1] != 0)
                fs_out[:, span] = jnp.where(outside, 0.0, slope).astype(BF16)
                if 0 <= layer < nz:
                    fg_out[:, layer * nx : (layer + 1) * nx] = total[c1 : c1 + c1 * ny]
    nine = 9 * c1
    slopes = fs_out[c1 : c1 + c1 * ny, nx : (nz + 1) * nx].astype(F32)
    shifted = [
        moved(slopes, nx, -1).astype(BF16), slopes.astype(BF16), moved(slopes, nx, 1).astype(BF16)
    ]
    total = None
    for y in range(ny):
        left = jnp.concatenate([s[y * c1 : (y + 1) * c1] for s in shifted], axis=0)
        right = []
        for a in range(3):
            span = slice((a + 2) * nx, (a + 2 + nz) * nx)
            for b in range(3):
                at = y + b - 1
                if at < 0:
                    right.append(xl[c1:, span])
                elif at >= ny:
                    right.append(xh[:c1, span])
                else:
                    right.append(xo[at * c1 : (at + 1) * c1, span])
        term = mm_t(left, jnp.concatenate(right, axis=0))
        total = term if total is None else total + term
    g_out[:three, :nine] = total
    slopes = cs_ref[edge : edge + hy * c2, 2 * half : (2 + hz) * half].astype(F32)
    shifted = [
        moved(slopes, half, -1).astype(BF16),
        slopes.astype(BF16),
        moved(slopes, half, 1).astype(BF16),
    ]
    total = None
    for y in range(hy):
        left = jnp.concatenate([s[y * c2 : (y + 1) * c2] for s in shifted], axis=0)
        right = [
            p_ref[(y + 2) * c1 : (y + 5) * c1, (a + 2) * half : (a + 2 + hz) * half]
            for a in range(3)
        ]
        term = mm_t(left, jnp.concatenate(right, axis=0))
        total = term if total is None else total + term
    g_out[three:, :nine] = total


def volume_grad_kernel(fs, fg, wt, out, *, c1, nz, ny, nx):
    swap_back = swap_matrix(c1, ny)
    for layer in range(nz):
        parts = None
        for dz in range(3):
            term = mm(wt[dz], fs[:, (layer + dz) * nx : (layer + dz + 1) * nx])
            parts = term if parts is None else parts + term
        total = fg[:, layer * nx : (layer + 1) * nx] + combine(parts, nx)
        out[:, layer] = mm(swap_back, total.astype(BF16)).reshape(c1, ny, nx).astype(BF16)


def finish_kernel(*refs, c1, c2, scale_fine, scale_coarse):
    parts, (fine, coarse) = refs[:-2], refs[-2:]
    total = tree_sum([part[...].astype(F32) for part in parts])
    for a in range(3):
        for b in range(3):
            lanes = slice((a * 3 + b) * c1, (a * 3 + b + 1) * c1)
            for c in range(3):
                at = (a * 3 + b) * 3 + c
                fine[at] = total[c * c1 : (c + 1) * c1, lanes] * scale_fine
                first = 3 * c1 + c * c2
                coarse[at] = total[first : first + c2, lanes] * scale_coarse


def tree_sum(values):
    while len(values) > 1:
        values = [values[i] + values[i + 1] for i in range(0, len(values), 2)]
    return values[0]


def shapes(*pairs):
    return [jax.ShapeDtypeStruct(shape, kind) for shape, kind in pairs]


def call(body, outs, args, flops=0, flags=False, scratch=(), name=None):
    specs = [pl.BlockSpec(memory_space=pltpu.VMEM) for _ in args]
    if flags:
        specs[0] = pl.BlockSpec(memory_space=pltpu.SMEM)
    nbytes = sum(a.size * a.dtype.itemsize for a in args)
    return pl.pallas_call(
        body,
        out_shape=outs,
        in_specs=specs,
        out_specs=[pl.BlockSpec(memory_space=pltpu.VMEM) for _ in outs],
        scratch_shapes=list(scratch),
        cost_estimate=pl.CostEstimate(flops=flops, bytes_accessed=nbytes, transcendentals=0),
        name=name,
    )(*args)


def shift_axis(value, axis, step):
    count = lax.axis_size(axis)
    pairs = [(i, i + step) for i in range(count) if 0 <= i + step < count]
    return lax.ppermute(value, axis, pairs)


def swap_bits(value, bits):
    ny = lax.axis_size("gy")
    count = lax.axis_size("gx") * ny
    flip = sum((bit if axis == "gy" else bit * ny) for axis, bit in bits)
    return lax.ppermute(value, ("gx", "gy"), [(i, i ^ flip) for i in range(count)])


def local(volume, fine_kernel, coarse_kernel, fine_cotangent, coarse_cotangent):
    c1, nz, ny, nx = volume.shape
    c2 = coarse_cotangent.shape[0]
    hz, hy, half = nz // 2, ny // 2, nx // 2
    gx, gy = lax.axis_size("gx"), lax.axis_size("gy")
    cells = nz * gx * ny * gy * nx
    at_x, at_y = lax.axis_index("gx"), lax.axis_index("gy")
    flags = jnp.stack([at_x == 0, at_x == gx - 1, at_y == 0, at_y == gy - 1]).astype(jnp.int32)
    sizes = dict(c1=c1, nz=nz, ny=ny, nx=nx)

    depth = 3
    vol_lo = shift_axis(volume[:, nz - depth :], "gx", 1)
    vol_hi = shift_axis(volume[:, :depth], "gx", -1)

    taps_f = fine_kernel.reshape(27 * c1, c1)
    taps_c = coarse_kernel.reshape(27 * c2, c1)
    flip_f = fine_kernel[::-1, ::-1, ::-1].swapaxes(3, 4).reshape(27 * c1, c1)
    flip_c = coarse_kernel[::-1, ::-1, ::-1].swapaxes(3, 4).reshape(27 * c1, c2)
    wa, wt, wc, wct = call(
        functools.partial(weights_kernel, c1=c1, c2=c2, ny=ny),
        shapes(
            ((3, 3 * (ny + 2) * c1, (ny + 4) * c1), BF16),
            ((3, 3 * ny * c1, (ny + 2) * c1), BF16),
            ((3, 3 * (hy + 4) * c2, (hy + 6) * c1), BF16),
            ((3, 3 * (hy + 2) * c1, (hy + 4) * c2), BF16),
        ),
        [taps_f, flip_f, taps_c, flip_c],
        flops=10**9,
        name="weights",
    )
    cot_c = coarse_cotangent.reshape(c2, hz * hy, half)
    cot_dn, cot_up = call(
        cot_pack_kernel,
        shapes(((2 * c1, ny, nx), BF16), ((2 * c1, ny, nx), BF16)),
        [fine_cotangent, cot_c],
        flops=10**8,
        name="cot_pack",
    )

    layers = nz + 2 * depth
    own, row_dn, row_up = call(
        rows_kernel,
        shapes(
            ((ny * c1, layers * nx), BF16),
            ((2 * c1, layers * nx), BF16),
            ((2 * c1, layers * nx), BF16),
        ),
        [volume, vol_lo, vol_hi],
        flops=10**9,
        name="rows",
    )
    cot_lo = shift_axis(cot_up, "gx", 1)
    cot_hi = shift_axis(cot_dn, "gx", -1)
    row_lo = shift_axis(row_up, "gy", 1)
    row_hi = shift_axis(row_dn, "gy", -1)

    fine_out, slopes, pz_dn, pz_up, pz_own = call(
        functools.partial(fine_kernel_fn, **sizes),
        shapes(
            ((c1, nz, ny, nx), BF16),
            (((ny + 2) * c1, (nz + 2) * nx), F32),
            ((hy * c1, (hz + 1) * half), BF16),
            ((hy * c1, (hz + 1) * half), BF16),
            ((hy * c1, hz * half), BF16),
        ),
        [flags, own, row_lo, row_hi, wa],
        flops=3 * 10**9,
        flags=True,
        name="fine",
    )
    pz_lo = shift_axis(pz_up, "gx", 1)
    pz_hi = shift_axis(pz_dn, "gx", -1)
    fcot, ccot, cy_dn, cy_up = call(
        functools.partial(cot_rows_kernel, c1=c1, c2=c2, ny=ny),
        shapes(
            ((ny * c1, (nz + 2) * nx), BF16),
            ((hy * c2, 3 * hz * half), BF16),
            ((2 * c2 + 2 * c1, 3 * hz * half), BF16),
            ((2 * c2 + 2 * c1, 3 * hz * half), BF16),
        ),
        [fine_cotangent, cot_c, cot_lo, cot_hi],
        flops=10**9,
        name="cot_rows",
    )
    cy_lo = shift_axis(cy_up, "gy", 1)
    cy_hi = shift_axis(cy_dn, "gy", -1)
    wide = (hz + 2 * (hz + 1)) * half
    py_dn, py_up = call(
        pooled_rows_kernel,
        shapes(((3 * c1, wide), BF16), ((3 * c1, wide), BF16)),
        [pz_lo, pz_own, pz_hi],
        flops=10**8,
        name="pooled_rows",
    )
    py_lo = shift_axis(py_up, "gy", 1)
    py_hi = shift_axis(py_dn, "gy", -1)

    coarse_out, fslope, fgrad, terms = call(
        functools.partial(coarse_kernel_fn, c2=c2, **sizes),
        shapes(
            ((c2 * hz * hy, half), BF16),
            (((ny + 2) * c1, (nz + 2) * nx), BF16),
            ((ny * c1, nz * nx), F32),
            ((3 * c1 + 3 * c2, 9 * c1), F32),
        ),
        [flags, pz_own, pz_lo, pz_hi, py_lo, py_hi, ccot, fcot, cy_lo, cy_hi, slopes]
        + [own, row_lo, row_hi, wc, wct],
        flops=4 * 10**9,
        flags=True,
        scratch=[
            pltpu.VMEM(((hy + 6) * c1, wide), BF16),
            pltpu.VMEM(((hy + 4) * c2, 3 * hz * half), BF16),
        ],
        name="coarse",
    )

    bits = [("gy", 1 << n) for n in range(gy.bit_length() - 1)]
    bits += [("gx", 1 << n) for n in range(gx.bit_length() - 1)]
    first = len(bits) % 2
    rounds = [bits[:1]] * first
    rounds += [bits[n : n + 2] for n in range(first, len(bits), 2)]
    value = terms
    for index, group in enumerate(rounds):
        if index:
            value = value.astype(BF16)
        parts = [value] + [swap_bits(value, [bit]) for bit in group]
        if len(group) == 2:
            parts.append(swap_bits(value, group))
        if index + 1 < len(rounds):
            value = tree_sum([part.astype(F32) for part in parts])
    (volume_grad,) = call(
        functools.partial(volume_grad_kernel, **sizes),
        shapes(((c1, nz, ny, nx), BF16)),
        [fslope, fgrad, wt],
        flops=2 * 10**9,
        name="volume_grad",
    )
    fine_grad, coarse_grad = call(
        functools.partial(
            finish_kernel,
            c1=c1,
            c2=c2,
            scale_fine=cells ** (-0.5),
            scale_coarse=(cells // 8) ** (-0.5),
        ),
        shapes(((27, c1, c1), F32), ((27, c2, c1), F32)),
        parts,
        flops=10**7,
        name="finish",
    )
    return (
        fine_out,
        coarse_out.reshape(c2, hz, hy, half),
        volume_grad,
        fine_grad.reshape(fine_kernel.shape),
        coarse_grad.reshape(coarse_kernel.shape),
    )


def solution(mesh):
    split = P(None, "gx", "gy", None)
    return jax.shard_map(
        local,
        mesh=mesh,
        in_specs=(split, P(), P(), split, split),
        out_specs=(split, split, split, P(), P()),
        check_vma=False,
    )
```

```python
import functools

import jax
import jax.numpy as jnp
from jax import lax
from jax.experimental import pallas as pl
from jax.experimental.pallas import tpu as pltpu
from jax.sharding import PartitionSpec as P

F32 = jnp.float32
BF16 = jnp.bfloat16


def mm(left, right):
    return jnp.dot(left, right, preferred_element_type=F32)


def mm_t(left, right):
    return lax.dot_general(left, right, (((1,), (1,)), ((), ())), preferred_element_type=F32)


def one_hot(shape, rule):
    rows = lax.broadcasted_iota(jnp.int32, shape, 0)
    cols = lax.broadcasted_iota(jnp.int32, shape, 1)
    return jnp.where(rule(rows, cols), 1.0, 0.0).astype(BF16)


def swap_matrix(outer, inner):
    count = outer * inner
    return one_hot((count, count), lambda r, c: c == (r % inner) * outer + r // inner)


def moved(values, width, offset):
    lanes = values.shape[1]
    place = lax.broadcasted_iota(jnp.int32, values.shape, 1) % width
    if offset == 1:
        return jnp.where(place == 0, 0.0, pltpu.roll(values, 1, 1))
    return jnp.where(place == width - 1, 0.0, pltpu.roll(values, lanes - 1, 1))


def combine(parts, width):
    rows = parts.shape[0] // 3
    return (
        parts[rows : 2 * rows]
        + moved(parts[:rows], width, 1)
        + moved(parts[2 * rows :], width, -1)
    )


def to_rows(values):
    chans, rows, width = values.shape
    return values.astype(F32).reshape(chans * rows, width).astype(BF16)


def band(taps_ref, out_ref, out_rows, turned, flipped):
    m, n = taps_ref.shape[1:][::-1] if turned else taps_ref.shape[1:]
    wide = (out_rows + 2) * n
    spread = one_hot((n, wide), lambda r, c: c % n == r)
    block = lax.broadcasted_iota(jnp.int32, (m, wide), 1) // n
    if turned:
        tiled = [
            lax.dot_general(
                taps_ref[at], spread, (((0,), (0,)), ((), ())), preferred_element_type=F32
            )
            for at in range(27)
        ]
    else:
        every = mm(taps_ref[...].reshape(27 * m, n), spread)
        tiled = [every[at * m : (at + 1) * m] for at in range(27)]
    if flipped:
        tiled = tiled[::-1]
    for a in range(3):
        for c in range(3):
            taps = [tiled[(a * 3 + b) * 3 + c] for b in range(3)]
            for y in range(out_rows):
                value = jnp.where(
                    block == y,
                    taps[0],
                    jnp.where(block == y + 1, taps[1], jnp.where(block == y + 2, taps[2], 0.0)),
                )
                start = (c * out_rows + y) * m
                out_ref[a, start : start + m, :] = value.astype(BF16)


def weights_kernel(kf, kc, wa, wt, wc, wct, *, ny):
    band(kf, wa, ny + 2, False, False)
    band(kf, wt, ny, True, True)
    band(kc, wc, ny // 2 + 4, True, False)
    band(kc, wct, ny // 2 + 2, False, True)


def ends():
    out = []
    for axis in ("gx", "gy"):
        at = lax.axis_index(axis)
        out.append((at % 2 == 0, at == 0, at == lax.axis_size(axis) - 1))
    return out


def volume_rows_kernel(vol, own, even, odd):
    c1, nz, ny, nx = vol.shape
    swap = swap_matrix(ny, c1)
    for z in range(nz):
        own[:, z * nx : (z + 1) * nx] = mm(swap, to_rows(vol[:, z])).astype(BF16)
    low, high = own[:, : even.shape[1]], own[:, own.shape[1] - even.shape[1] :]
    first = ends()[0][0]
    even[...] = jnp.where(first, high, low)
    odd[...] = jnp.where(first, low, high)


def cot_rows_kernel(fc, cc, fine, coarse, even, odd):
    c1, nz, ny, nx = fc.shape
    c2, cells, half = cc.shape
    hy = ny // 2
    swap = swap_matrix(ny, c1)
    for z in range(nz):
        fine[:, z * nx : (z + 1) * nx] = mm(swap, to_rows(fc[:, z])).astype(BF16)
    rows = mm(swap_matrix(cells, c2), to_rows(cc[...])).astype(BF16)
    for z in range(cells // hy):
        coarse[:, z * half : (z + 1) * half] = rows[z * hy * c2 : (z + 1) * hy * c2]
    first = ends()[0][0]
    low, high = fine[:, :nx], fine[:, (nz - 1) * nx :]
    even[:, :nx] = jnp.where(first, high, low)
    odd[:, :nx] = jnp.where(first, low, high)
    even[:, nx:] = coarse[...]
    odd[:, nx:] = coarse[...]


def stack_layers(out, own, even, odd, lanes):
    first = ends()[0][0]
    width = lanes.stop - lanes.start
    low, high = even[:, lanes], odd[:, lanes]
    out[:, :width] = jnp.where(first, high, low)
    out[:, width : width + own.shape[1]] = own[...]
    out[:, width + own.shape[1] :] = jnp.where(first, low, high)


def volume_layers_kernel(own, z_even, z_odd, out, even, odd):
    stack_layers(out, own, z_even, z_odd, slice(0, z_even.shape[1]))
    edge = even.shape[0]
    first = ends()[1][0]
    low, high = out[:edge], out[out.shape[0] - edge :]
    even[...] = jnp.where(first, high, low)
    odd[...] = jnp.where(first, low, high)


def coarse_layers_kernel(po, pz_even, pz_odd, fo, co, cz_even, cz_odd, p_out, f_out, c_out, even, odd):
    nx = cz_even.shape[1] - co.shape[1]
    stack_layers(p_out, po, pz_even, pz_odd, slice(0, pz_even.shape[1]))
    stack_layers(f_out, fo, cz_even, cz_odd, slice(0, nx))
    stack_layers(c_out, co, cz_even, cz_odd, slice(nx, cz_even.shape[1]))
    three = even.shape[0]
    c1 = three // 3
    pooled, wide = p_out.shape[1], c_out.shape[1]
    first = ends()[1][0]

    def put(rows, lanes, low, high):
        even[rows, lanes] = jnp.where(first, high, low)
        odd[rows, lanes] = jnp.where(first, low, high)

    def tail(ref, count):
        return slice(ref.shape[0] - count, ref.shape[0])

    put(slice(0, three), slice(0, pooled), p_out[:three], p_out[tail(p_out, three)])
    near = slice(pooled, pooled + wide)
    far = slice(pooled + wide, pooled + 2 * wide)
    low, high = c_out[: 4 * c1], c_out[tail(c_out, 4 * c1)]
    put(slice(0, three), near, low[:three], high[:three])
    put(slice(0, c1), far, low[three:], high[three:])
    low, high = f_out[:c1], f_out[tail(f_out, c1)]
    put(slice(c1, 2 * c1), far, low[:, :wide], high[:, :wide])
    put(slice(2 * c1, three), far, low[:, wide:], high[:, wide:])


def weight_rows(w_ref, dz, first, count):
    rows = w_ref.shape[1] // 3
    return jnp.concatenate(
        [w_ref[dz, c * rows + first : c * rows + first + count] for c in range(3)], axis=0
    )


def fine_kernel_fn(xo, y_even, y_odd, wa, x_ref, pre_out, fo_out, pz_even, pz_odd, pz_own, *, c1, nz, ny, nx):
    (first_x, start_x, stop_x), (first_y, _, _) = ends()
    low, high = y_even[...], y_odd[...]
    x_ref[: 2 * c1] = jnp.where(first_y, high, low)
    x_ref[2 * c1 : 2 * c1 + c1 * ny] = xo[...]
    x_ref[2 * c1 + c1 * ny :] = jnp.where(first_y, low, high)
    pool = one_hot((nx, nx // 2), lambda r, c: r // 2 == c)
    cells = []
    sums = None
    weights = [weight_rows(wa, dz, c1, c1 * ny) for dz in range(3)]
    for layer in range(nz + 4):
        parts = None
        for dz in range(3):
            term = mm(weights[dz], x_ref[:, (layer + dz) * nx : (layer + dz + 1) * nx])
            parts = term if parts is None else parts + term
        pre = combine(parts, nx)
        sig = jax.nn.sigmoid(pre)
        span = slice((layer + 1) * nx, (layer + 2) * nx)
        fo = (xo[:, span].astype(F32) + pre * sig).astype(BF16)
        if 1 <= layer <= nz + 2:
            pre_out[:, (layer - 1) * nx : layer * nx] = pre
        if 2 <= layer < nz + 2:
            fo_out[:, (layer - 2) * nx : (layer - 1) * nx] = fo
        pooled = mm(fo, pool)
        if layer % 2 == 0:
            sums = pooled
            continue
        sums = sums + pooled
        rows = [
            sums[2 * r * c1 : (2 * r + 1) * c1] + sums[(2 * r + 1) * c1 : (2 * r + 2) * c1]
            for r in range(ny // 2)
        ]
        value = jnp.concatenate(rows, axis=0) * 0.125
        place = layer // 2
        last = nz // 2 + 1
        if place == 0:
            value = jnp.where(start_x, 0.0, value)
        if place == last:
            value = jnp.where(stop_x, 0.0, value)
        cells.append(value.astype(BF16))
    pz_own[...] = jnp.concatenate(cells[1:-1], axis=1)
    low, high = jnp.concatenate(cells[1:], axis=1), jnp.concatenate(cells[:-1], axis=1)
    pz_even[...] = jnp.where(first_x, high, low)
    pz_odd[...] = jnp.where(first_x, low, high)


def slope_kernel_fn(x_ref, wa, pre_ref, fo, fo_out, sl_out, *, c1, nz, ny, nx):
    swap_back = swap_matrix(c1, ny)
    low = [weight_rows(wa, dz, 0, c1) for dz in range(3)]
    high = [weight_rows(wa, dz, c1 + c1 * ny, c1) for dz in range(3)]
    for layer in range(nz + 2):
        edges = []
        for weights in (low, high):
            parts = None
            for dz in range(3):
                term = mm(weights[dz], x_ref[:, (layer + 1 + dz) * nx : (layer + 2 + dz) * nx])
                parts = term if parts is None else parts + term
            edges.append(combine(parts, nx))
        span = slice(layer * nx, (layer + 1) * nx)
        pre = jnp.concatenate([edges[0], pre_ref[:, span], edges[1]], axis=0)
        sig = jax.nn.sigmoid(pre)
        sl_out[:, span] = sig * (1.0 + pre * (1.0 - sig))
    for layer in range(nz):
        rows = mm(swap_back, fo[:, layer * nx : (layer + 1) * nx])
        fo_out[:, layer] = rows.reshape(c1, ny, nx).astype(BF16)


def coarse_kernel_fn(
    po, fc, cc, y_even, y_odd, sl, x_ref, wc, wct,
    co_out, fs_out, fg_out, g_out, p_ref, cs_ref, edge_ref, *, c1, c2, nz, ny, nx,
):
    half, hz, hy = nx // 2, nz // 2, ny // 2
    three = 3 * c1
    (_, start_x, stop_x), (first_y, start_y, stop_y) = ends()
    low, high = y_even[...], y_odd[...]
    edge_ref[0] = jnp.where(first_y, high, low)
    edge_ref[1] = jnp.where(first_y, low, high)
    pooled, wide = po.shape[1], cc.shape[1]
    p_ref[:three] = edge_ref[0, :, :pooled]
    p_ref[three : three + hy * c1] = po[...]
    p_ref[three + hy * c1 :] = edge_ref[1, :, :pooled]
    edge = 2 * c2
    swap_c = swap_matrix(c2, hz * hy)
    for pair in range((hz + 4) // 2):
        parts = None
        for dz in range(3):
            first = (2 * pair + dz) * half
            term = mm(wc[dz], p_ref[:, first : first + nx])
            parts = term if parts is None else parts + term
        pre = combine(parts, half)
        sig = jax.nn.sigmoid(pre)
        span = slice(pair * nx, (pair + 1) * nx)
        near = slice(pooled + pair * nx, pooled + (pair + 1) * nx)
        far = slice(pooled + wide + pair * nx, pooled + wide + (pair + 1) * nx)
        cot = jnp.concatenate(
            [
                edge_ref[0, :, near],
                edge_ref[0, :c1, far],
                cc[:, span],
                edge_ref[1, :, near],
                edge_ref[1, :c1, far],
            ],
            axis=0,
        )
        cs_ref[:, span] = (cot.astype(F32) * (sig * (1.0 + pre * (1.0 - sig)))).astype(BF16)
        if pair == 1:
            inner = slice(edge, edge + hy * c2)
            out = (pre[inner] * sig[inner]).astype(BF16)
            stacked = jnp.concatenate([out[:, :half], out[:, half:]], axis=0)
            co_out[...] = mm(swap_c, stacked).astype(BF16)
    widen = one_hot((half, nx), lambda r, c: c // 2 == r)
    base = pooled + wide
    for pair in range((hz + 2) // 2):
        parts = None
        for dz in range(3):
            first = (2 * pair + dz) * half
            term = mm(wct[dz], cs_ref[:, first : first + nx])
            parts = term if parts is None else parts + term
        grad = combine(parts, half) * 0.125
        high = grad.astype(BF16)
        low = (grad - high.astype(F32)).astype(BF16)
        for side in range(2):
            lanes = slice(side * half, (side + 1) * half)
            up = mm(high[:, lanes], widen) + mm(low[:, lanes], widen)
            blocks = [up[(y + 2) // 2 * c1 : (y + 2) // 2 * c1 + c1] for y in range(-1, ny + 1)]
            spread = jnp.concatenate(blocks, axis=0)
            coarse_layer = 2 * pair + side - 1
            for layer in (2 * coarse_layer, 2 * coarse_layer + 1):
                if not -1 <= layer <= nz:
                    continue
                place = layer + 1
                span = slice(place * nx, (place + 1) * nx)
                fold = place * nx // wide
                first = base + place * nx - fold * wide
                inside = slice(first, first + nx)
                rows = slice((fold + 1) * c1, (fold + 2) * c1)
                cot = jnp.concatenate(
                    [edge_ref[0, rows, inside], fc[:, span], edge_ref[1, rows, inside]], axis=0
                )
                total = cot.astype(F32) + spread
                slope = total * sl[:, span]
                row = lax.broadcasted_iota(jnp.int32, slope.shape, 0) // c1
                outside = jnp.logical_and(row == 0, start_y)
                outside = jnp.logical_or(outside, jnp.logical_and(row == ny + 1, stop_y))
                if layer == -1:
                    outside = jnp.logical_or(outside, start_x)
                if layer == nz:
                    outside = jnp.logical_or(outside, stop_x)
                fs_out[:, span] = jnp.where(outside, 0.0, slope).astype(BF16)
                if 0 <= layer < nz:
                    fg_out[:, layer * nx : (layer + 1) * nx] = total[c1 : c1 + c1 * ny]
    slopes = fs_out[c1 : c1 + c1 * ny, nx : (nz + 1) * nx].astype(F32)
    shifted = [
        moved(slopes, nx, -1).astype(BF16), slopes.astype(BF16), moved(slopes, nx, 1).astype(BF16)
    ]
    fine = None
    for y in range(ny):
        left = jnp.concatenate([s[y * c1 : (y + 1) * c1] for s in shifted], axis=0)
        right = [
            x_ref[(y + 1) * c1 : (y + 4) * c1, (a + 2) * nx : (a + 2 + nz) * nx] for a in range(3)
        ]
        term = mm_t(left, jnp.concatenate(right, axis=0))
        fine = term if fine is None else fine + term
    slopes = cs_ref[edge : edge + hy * c2, 2 * half : (2 + hz) * half].astype(F32)
    shifted = [
        moved(slopes, half, -1).astype(BF16),
        slopes.astype(BF16),
        moved(slopes, half, 1).astype(BF16),
    ]
    coarse = None
    for y in range(hy):
        left = jnp.concatenate([s[y * c2 : (y + 1) * c2] for s in shifted], axis=0)
        right = [
            p_ref[(y + 2) * c1 : (y + 5) * c1, (a + 2) * half : (a + 2 + hz) * half]
            for a in range(3)
        ]
        term = mm_t(left, jnp.concatenate(right, axis=0))
        coarse = term if coarse is None else coarse + term
    g_out[:three, :] = fine[:, : 8 * c1]
    g_out[three : 9 * c1, :] = coarse[:, : 8 * c1]
    last = [fine[:, 8 * c1 :], coarse[:, 8 * c1 :]]
    last = jnp.concatenate(last, axis=0)
    groups = [last[r * c1 : (r + 1) * c1] for r in range(9)]
    g_out[9 * c1 : 10 * c1, :] = jnp.concatenate(groups[:8], axis=1)
    g_out[10 * c1 :, :] = jnp.concatenate([groups[8]] * 8, axis=1)


def volume_grad_kernel(fs, fg, wt, out, *, c1, nz, ny, nx):
    swap_back = swap_matrix(c1, ny)
    for layer in range(nz):
        parts = None
        for dz in range(3):
            term = mm(wt[dz], fs[:, (layer + dz) * nx : (layer + dz + 1) * nx])
            parts = term if parts is None else parts + term
        total = fg[:, layer * nx : (layer + 1) * nx] + combine(parts, nx)
        out[:, layer] = mm(swap_back, total.astype(BF16)).reshape(c1, ny, nx).astype(BF16)


def finish_kernel(*refs, c1, c2, scale_fine, scale_coarse):
    parts, (fine, coarse) = refs[:-2], refs[-2:]
    total = tree_sum([part[...].astype(F32) for part in parts])
    tail = total[9 * c1 :]
    groups = [tail[:c1, r * c1 : (r + 1) * c1] for r in range(8)] + [tail[c1:, :c1]]
    last = jnp.concatenate(groups, axis=0)
    for c in range(3):
        own = slice(c * c1, (c + 1) * c1)
        for ab in range(8):
            fine[ab * 3 + c] = total[own, ab * c1 : (ab + 1) * c1] * scale_fine
        fine[24 + c] = last[own] * scale_fine
    for part, taps in ((total[3 * c1 : 9 * c1], 8), (last[3 * c1 :], 1)):
        turned = part.T * scale_coarse
        for ab in range(taps):
            for c in range(3):
                at = (8 if taps == 1 else ab) * 3 + c
                coarse[at] = turned[ab * c1 : (ab + 1) * c1, c * c2 : (c + 1) * c2]


def tree_sum(values):
    while len(values) > 1:
        values = [values[i] + values[i + 1] for i in range(0, len(values), 2)]
    return values[0]


def shapes(*pairs):
    return [pltpu.VMEM(shape, kind) for shape, kind in pairs]


def result(shape, kind):
    return jax.ShapeDtypeStruct(shape, kind)


def call(body, outs, args, flops=0, scratch=(), name=None):
    specs = [pl.BlockSpec(memory_space=pltpu.VMEM) for _ in args]
    nbytes = sum(a.size * a.dtype.itemsize for a in args)
    placed = [pltpu.with_memory_space_constraint(arg, pltpu.VMEM) for arg in args]
    return pl.pallas_call(
        body,
        out_shape=outs,
        in_specs=specs,
        out_specs=[pl.BlockSpec(memory_space=pltpu.VMEM) for _ in outs],
        scratch_shapes=list(scratch),
        compiler_params=pltpu.CompilerParams(vmem_limit_bytes=24 * 2**20),
        cost_estimate=pl.CostEstimate(flops=flops, bytes_accessed=nbytes, transcendentals=0),
        name=name,
    )(*placed)


def swap_pairs(even, odd, axis):
    count = lax.axis_size(axis)
    out = []
    for value, first in ((even, 0), (odd, 1)):
        pairs = [(i, i + 1) for i in range(first, count - 1, 2)]
        pairs += [(target, source) for source, target in pairs]
        out.append(lax.ppermute(value, axis, pairs))
    return out


def swap_bits(value, bits):
    ny = lax.axis_size("gy")
    count = lax.axis_size("gx") * ny
    flip = sum((bit if axis == "gy" else bit * ny) for axis, bit in bits)
    return lax.ppermute(value, ("gx", "gy"), [(i, i ^ flip) for i in range(count)])


def local(volume, fine_kernel, coarse_kernel, fine_cotangent, coarse_cotangent):
    c1, nz, ny, nx = volume.shape
    c2 = coarse_cotangent.shape[0]
    hz, hy, half = nz // 2, ny // 2, nx // 2
    gx, gy = lax.axis_size("gx"), lax.axis_size("gy")
    cells = nz * gx * ny * gy * nx
    sizes = dict(c1=c1, nz=nz, ny=ny, nx=nx)
    depth = 3
    rows, half_rows = ny * c1, hy * c1

    own, z_even, z_odd = call(
        volume_rows_kernel,
        shapes(((rows, nz * nx), BF16), ((rows, depth * nx), BF16), ((rows, depth * nx), BF16)),
        [volume],
        flops=10**8,
        name="volume_rows",
    )
    z_even, z_odd = swap_pairs(z_even, z_odd, "gx")
    wa, wt, wc, wct = call(
        functools.partial(weights_kernel, ny=ny),
        shapes(
            ((3, 3 * (ny + 2) * c1, (ny + 4) * c1), BF16),
            ((3, 3 * ny * c1, (ny + 2) * c1), BF16),
            ((3, 3 * (hy + 4) * c2, (hy + 6) * c1), BF16),
            ((3, 3 * (hy + 2) * c1, (hy + 4) * c2), BF16),
        ),
        [
            fine_kernel.reshape(27, c1, c1),
            coarse_kernel.swapaxes(3, 4).reshape(27, c1, c2),
        ],
        flops=10**9,
        name="weights",
    )
    fine_cot, coarse_cot, cz_even, cz_odd = call(
        cot_rows_kernel,
        shapes(
            ((rows, nz * nx), BF16),
            ((hy * c2, hz * half), BF16),
            ((rows, nx + hz * half), BF16),
            ((rows, nx + hz * half), BF16),
        ),
        [fine_cotangent, coarse_cotangent.reshape(c2, hz * hy, half)],
        flops=10**8,
        name="cot_rows",
    )

    layers = (nz + 2 * depth) * nx
    own, y_even, y_odd = call(
        volume_layers_kernel,
        shapes(((rows, layers), BF16), ((2 * c1, layers), BF16), ((2 * c1, layers), BF16)),
        [own, z_even, z_odd],
        flops=10**8,
        name="volume_layers",
    )
    y_even, y_odd = swap_pairs(y_even, y_odd, "gy")
    cz_even, cz_odd = swap_pairs(cz_even, cz_odd, "gx")

    volume_rows, pre, fine_rows, pz_even, pz_odd, pz_own = call(
        functools.partial(fine_kernel_fn, **sizes),
        shapes(
            ((rows + 4 * c1, layers), BF16),
            ((rows, (nz + 2) * nx), F32),
            ((rows, nz * nx), BF16),
            ((half_rows, (hz + 1) * half), BF16),
            ((half_rows, (hz + 1) * half), BF16),
            ((half_rows, hz * half), BF16),
        ),
        [own, y_even, y_odd, wa],
        flops=3 * 10**9,
        name="fine",
    )
    pz_even, pz_odd = swap_pairs(pz_even, pz_odd, "gx")
    fine_out, slopes = call(
        functools.partial(slope_kernel_fn, **sizes),
        [result((c1, nz, ny, nx), BF16)] + shapes(((rows + 2 * c1, (nz + 2) * nx), F32)),
        [volume_rows, wa, pre, fine_rows],
        flops=2 * 10**9,
        name="slopes",
    )
    pooled_lanes = (3 * hz + 2) * half
    cot_lanes = 3 * hz * half
    sent = (3 * c1, pooled_lanes + 2 * cot_lanes)
    pooled, fine_cot, coarse_cot, y_even, y_odd = call(
        coarse_layers_kernel,
        shapes(
            ((half_rows, pooled_lanes), BF16),
            ((rows, (nz + 2) * nx), BF16),
            ((hy * c2, cot_lanes), BF16),
            (sent, BF16),
            (sent, BF16),
        ),
        [pz_own, pz_even, pz_odd, fine_cot, coarse_cot, cz_even, cz_odd],
        flops=10**8,
        name="coarse_layers",
    )
    y_even, y_odd = swap_pairs(y_even, y_odd, "gy")

    coarse_out, fslope, fgrad, terms = call(
        functools.partial(coarse_kernel_fn, c2=c2, **sizes),
        shapes(
            ((c2 * hz * hy, half), BF16),
            ((rows + 2 * c1, (nz + 2) * nx), BF16),
            ((rows, nz * nx), F32),
            ((11 * c1, 8 * c1), F32),
        ),
        [pooled, fine_cot, coarse_cot, y_even, y_odd, slopes, volume_rows, wc, wct],
        flops=4 * 10**9,
        scratch=[
            pltpu.VMEM(((hy + 6) * c1, pooled_lanes), BF16),
            pltpu.VMEM(((hy + 4) * c2, cot_lanes), BF16),
            pltpu.VMEM((2,) + sent, BF16),
        ],
        name="coarse",
    )

    bits = [("gy", 1 << n) for n in range(gy.bit_length() - 1)]
    bits += [("gx", 1 << n) for n in range(gx.bit_length() - 1)]
    first = len(bits) % 2
    rounds = [bits[:1]] * first
    rounds += [bits[n : n + 2] for n in range(first, len(bits), 2)]
    value = terms
    for index, group in enumerate(rounds):
        if index:
            value = value.astype(BF16)
        parts = [value] + [swap_bits(value, [bit]) for bit in group]
        if len(group) == 2:
            parts.append(swap_bits(value, group))
        if index + 1 < len(rounds):
            value = tree_sum([part.astype(F32) for part in parts])
    (volume_grad,) = call(
        functools.partial(volume_grad_kernel, **sizes),
        [result((c1, nz, ny, nx), BF16)],
        [fslope, fgrad, wt],
        flops=2 * 10**9,
        name="volume_grad",
    )
    fine_grad, coarse_grad = call(
        functools.partial(
            finish_kernel,
            c1=c1,
            c2=c2,
            scale_fine=cells ** (-0.5),
            scale_coarse=(cells // 8) ** (-0.5),
        ),
        [result((27, c1, c1), F32), result((27, c1, c2), F32)],
        parts,
        flops=10**7,
        name="finish",
    )
    return (
        fine_out,
        coarse_out.reshape(c2, hz, hy, half),
        volume_grad,
        fine_grad.reshape(fine_kernel.shape),
        coarse_grad.reshape(3, 3, 3, c1, c2).swapaxes(3, 4),
    )


def solution(mesh):
    split = P(None, "gx", "gy", None)
    return jax.shard_map(
        local,
        mesh=mesh,
        in_specs=(split, P(), P(), split, split),
        out_specs=(split, split, split, P(), P()),
        check_vma=False,
    )
```

```python
import functools

import jax
import jax.numpy as jnp
from jax import lax
from jax.experimental import pallas as pl
from jax.experimental.pallas import tpu as pltpu
from jax.sharding import PartitionSpec as P


F32 = jnp.float32
BF16 = jnp.bfloat16


def mm(left, right):
    return jnp.dot(left, right, preferred_element_type=F32)


def mm_t(left, right):
    return lax.dot_general(left, right, (((1,), (1,)), ((), ())), preferred_element_type=F32)


def one_hot(shape, rule):
    rows = lax.broadcasted_iota(jnp.int32, shape, 0)
    cols = lax.broadcasted_iota(jnp.int32, shape, 1)
    return jnp.where(rule(rows, cols), 1.0, 0.0).astype(BF16)


def swap_matrix(outer, inner):
    count = outer * inner
    return one_hot((count, count), lambda r, c: c == (r % inner) * outer + r // inner)


def moved(values, width, offset):
    lanes = values.shape[1]
    place = lax.broadcasted_iota(jnp.int32, values.shape, 1) % width
    if offset == 1:
        return jnp.where(place == 0, 0.0, pltpu.roll(values, 1, 1))
    return jnp.where(place == width - 1, 0.0, pltpu.roll(values, lanes - 1, 1))


def combine(parts, width):
    rows = parts.shape[0] // 3
    return (
        parts[rows : 2 * rows]
        + moved(parts[:rows], width, 1)
        + moved(parts[2 * rows :], width, -1)
    )


def to_rows(values):
    chans, rows, width = values.shape
    return values.astype(F32).reshape(chans * rows, width).astype(BF16)


def band(taps_ref, out_ref, out_rows, turned, flipped):
    m, n = taps_ref.shape[1:][::-1] if turned else taps_ref.shape[1:]
    wide = (out_rows + 2) * n
    spread = one_hot((n, wide), lambda r, c: c % n == r)
    block = lax.broadcasted_iota(jnp.int32, (m, wide), 1) // n
    if turned:
        tiled = [
            lax.dot_general(
                taps_ref[at], spread, (((0,), (0,)), ((), ())), preferred_element_type=F32
            )
            for at in range(27)
        ]
    else:
        every = mm(taps_ref[...].reshape(27 * m, n), spread)
        tiled = [every[at * m : (at + 1) * m] for at in range(27)]
    if flipped:
        tiled = tiled[::-1]
    for a in range(3):
        for c in range(3):
            taps = [tiled[(a * 3 + b) * 3 + c] for b in range(3)]
            for y in range(out_rows):
                value = jnp.where(
                    block == y,
                    taps[0],
                    jnp.where(block == y + 1, taps[1], jnp.where(block == y + 2, taps[2], 0.0)),
                )
                start = (c * out_rows + y) * m
                out_ref[start : start + m, a * wide : (a + 1) * wide] = value.astype(BF16)


def weights_kernel(kf, kc, wa, wt, wc, wct, *, ny):
    band(kf, wa, ny, False, False)
    band(kf, wt, ny, True, True)
    band(kc, wc, ny // 2 + 2, True, False)
    band(kc, wct, ny // 2, False, True)


def ends():
    return [lax.axis_index(axis) % 2 == 0 for axis in ("gx", "gy")]


def volume_rows_kernel(vol, own, even, odd):
    c1, nz, ny, nx = vol.shape
    swap = swap_matrix(ny, c1)
    for z in range(nz):
        own[:, z * nx : (z + 1) * nx] = mm(swap, to_rows(vol[:, z])).astype(BF16)
    low, high = own[:, : even.shape[1]], own[:, own.shape[1] - even.shape[1] :]
    first = ends()[0]
    even[...] = jnp.where(first, high, low)
    odd[...] = jnp.where(first, low, high)


def cot_rows_kernel(fc, cc, fine, coarse):
    c1, nz, ny, nx = fc.shape
    c2, cells, half = cc.shape
    hy = ny // 2
    swap = swap_matrix(ny, c1)
    for z in range(nz):
        fine[:, z * nx : (z + 1) * nx] = mm(swap, to_rows(fc[:, z])).astype(BF16)
    rows = mm(swap_matrix(cells, c2), to_rows(cc[...])).astype(BF16)
    for z in range(cells // hy):
        coarse[:, z * half : (z + 1) * half] = rows[z * hy * c2 : (z + 1) * hy * c2]


def stack_layers(out, own, even, odd):
    first = ends()[0]
    width = even.shape[1]
    low, high = even[...], odd[...]
    out[:, :width] = jnp.where(first, high, low)
    out[:, width : width + own.shape[1]] = own[...]
    out[:, width + own.shape[1] :] = jnp.where(first, low, high)


def stack_rows(out, own, even, odd):
    first = ends()[1]
    edge = even.shape[0]
    low, high = even[...], odd[...]
    out[:edge] = jnp.where(first, high, low)
    out[edge : edge + own.shape[0]] = own[...]
    out[edge + own.shape[0] :] = jnp.where(first, low, high)


def layers_kernel(own, z_even, z_odd, out, even, odd):
    stack_layers(out, own, z_even, z_odd)
    edge = even.shape[0]
    first = ends()[1]
    low, high = out[:edge], out[out.shape[0] - edge :]
    even[...] = jnp.where(first, high, low)
    odd[...] = jnp.where(first, low, high)


def coarse_layers_kernel(po, co, z_even, z_odd, p_out, c_out, even, odd):
    lanes, rows = po.shape[1], po.shape[0]
    half = (z_even.shape[1] - lanes) // 2
    stack_layers(p_out, po, z_even.at[:, :lanes], z_odd.at[:, :lanes])
    first = ends()[0]
    width = co.shape[1]
    for part in range(2):
        span = slice(lanes + part * half, lanes + (part + 1) * half)
        low, high = z_even[:, span], z_odd[:, span]
        into = slice(part * rows, (part + 1) * rows)
        c_out[into, :half] = jnp.where(first, high, low)
        c_out[into, half + width :] = jnp.where(first, low, high)
    c_out[:, half : half + width] = co[...]
    edge = even.shape[0]
    pooled = p_out.shape[1]
    first = ends()[1]
    for ref, span in ((p_out, slice(0, pooled)), (c_out, slice(pooled, even.shape[1]))):
        low, high = ref[:edge], ref[ref.shape[0] - edge :]
        even[:, span] = jnp.where(first, high, low)
        odd[:, span] = jnp.where(first, low, high)


def three_layers(ref, rows, first, step, width):
    return jnp.concatenate(
        [ref[rows, first + dz * step : first + dz * step + width] for dz in range(3)], axis=0
    )


def fine_kernel_fn(xo, y_even, y_odd, wa, co, x_ref, pre_out, fo_out, po, z_even, z_odd, *, nz, nx):
    c1 = y_even.shape[0]
    half = nx // 2
    stack_rows(x_ref, xo, y_even, y_odd)
    pool = one_hot((nx, half), lambda r, c: r // 2 == c)
    rows = xo.shape[0]
    for layer in range(nz):
        parts = mm(wa[...], three_layers(x_ref, slice(None), layer * nx, nx, nx))
        pre = combine(parts, nx)
        pre_out[:, layer * nx : (layer + 1) * nx] = pre
        value = xo[:, (layer + 1) * nx : (layer + 2) * nx].astype(F32)
        fo = (value + pre * jax.nn.sigmoid(pre)).astype(BF16)
        fo_out[:, layer * nx : (layer + 1) * nx] = fo
        pooled = mm(fo, pool)
        if layer % 2 == 0:
            sums = pooled
            continue
        sums = sums + pooled
        cells = [
            sums[2 * r * c1 : (2 * r + 1) * c1] + sums[(2 * r + 1) * c1 : (2 * r + 2) * c1]
            for r in range(rows // c1 // 2)
        ]
        place = layer // 2
        value = jnp.concatenate(cells, axis=0) * 0.125
        po[:, place * half : (place + 1) * half] = value.astype(BF16)
    lanes = po.shape[1]
    low, high = co[:, :half], co[:, co.shape[1] - half :]
    first = ends()[0]
    for ref, value in (
        (z_even, jnp.where(first, high, low)),
        (z_odd, jnp.where(first, low, high)),
    ):
        ref[:, :lanes] = po[...]
        ref[:, lanes : lanes + half] = value[: rows // 2]
        ref[:, lanes + half :] = value[rows // 2 :]


def slope_kernel_fn(pre_ref, fo, fo_out, sl_out, *, c1, nz, ny, nx):
    swap_back = swap_matrix(c1, ny)
    for layer in range(nz):
        span = slice(layer * nx, (layer + 1) * nx)
        pre = pre_ref[:, span]
        sig = jax.nn.sigmoid(pre)
        sl_out[:, span] = sig * (1.0 + pre * (1.0 - sig))
        rows = mm(swap_back, fo[:, span])
        fo_out[:, layer] = rows.reshape(c1, ny, nx).astype(BF16)


def coarse_kernel_fn(
    po, cc, y_even, y_odd, fc, sl, wc, wct,
    p_ref, cs_ref, co_out, fs_out, fg_out, z_even, z_odd, c_ref, *, c1, c2, nz, ny, nx,
):
    half, hz, hy = nx // 2, nz // 2, ny // 2
    pooled = po.shape[1]
    stack_rows(p_ref, po, y_even.at[:, :pooled], y_odd.at[:, :pooled])
    stack_rows(c_ref, cc, y_even.at[:, pooled:], y_odd.at[:, pooled:])
    inner = slice(c2, c2 + hy * c2)
    own = []
    for pair in range((hz + 2) // 2):
        pre = combine(mm(wc[...], three_layers(p_ref, slice(None), pair * nx, half, nx)), half)
        sig = jax.nn.sigmoid(pre)
        span = slice(pair * nx, (pair + 1) * nx)
        cot = c_ref[:, span].astype(F32)
        cs_ref[:, span] = (cot * (sig * (1.0 + pre * (1.0 - sig)))).astype(BF16)
        out = (pre[inner] * sig[inner]).astype(BF16)
        own += [out[:, :half], out[:, half:]]
    stacked = jnp.concatenate(own[1:-1], axis=0)
    co_out[...] = mm(swap_matrix(c2, hz * hy), stacked).astype(BF16)
    widen = one_hot((half, nx), lambda r, c: c // 2 == r)
    for pair in range(hz // 2):
        parts = mm(wct[...], three_layers(cs_ref, slice(None), pair * nx, half, nx))
        grad = combine(parts, half) * 0.125
        high = grad.astype(BF16)
        low = (grad - high.astype(F32)).astype(BF16)
        for side in range(2):
            lanes = slice(side * half, (side + 1) * half)
            up = mm(high[:, lanes], widen) + mm(low[:, lanes], widen)
            blocks = [up[y // 2 * c1 : y // 2 * c1 + c1] for y in range(ny)]
            spread = jnp.concatenate(blocks, axis=0)
            for layer in (4 * pair + 2 * side, 4 * pair + 2 * side + 1):
                span = slice(layer * nx, (layer + 1) * nx)
                total = fc[:, span].astype(F32) + spread
                fg_out[:, span] = total
                fs_out[:, span] = (total * sl[:, span]).astype(BF16)
    low, high = fs_out[:, :nx], fs_out[:, (nz - 1) * nx :]
    first = ends()[0]
    z_even[...] = jnp.where(first, high, low)
    z_odd[...] = jnp.where(first, low, high)


def terms_of(slopes, cells, chans, count, width, rows, lanes):
    slopes = slopes.astype(F32)
    shifted = [moved(slopes, width, -1), slopes, moved(slopes, width, 1)]
    shifted = [value.astype(BF16) for value in shifted]
    total = None
    for y in range(slopes.shape[0] // chans):
        left = jnp.concatenate([s[y * chans : (y + 1) * chans] for s in shifted], axis=0)
        first = y * count + rows
        right = [
            cells[first : first + 3 * count, lanes + a * width : lanes + a * width + slopes.shape[1]]
            for a in range(3)
        ]
        term = mm_t(left, jnp.concatenate(right, axis=0))
        total = term if total is None else total + term
    return total


def terms_kernel(x_ref, fs, p_ref, cs, g_out, *, c1, c2, nx):
    half = nx // 2
    fine = terms_of(fs[...], x_ref, c1, c1, nx, 0, 0)
    inner = cs[c2 : cs.shape[0] - c2, half : cs.shape[1] - half]
    coarse = terms_of(inner, p_ref, c2, c1, half, c1, half)
    three = 3 * c1
    g_out[:three, :] = fine[:, : 8 * c1]
    g_out[three : 9 * c1, :] = coarse[:, : 8 * c1]
    last = jnp.concatenate([fine[:, 8 * c1 :], coarse[:, 8 * c1 :]], axis=0)
    groups = [last[r * c1 : (r + 1) * c1] for r in range(9)]
    g_out[9 * c1 : 10 * c1, :] = jnp.concatenate(groups[:8], axis=1)
    g_out[10 * c1 :, :] = jnp.concatenate([groups[8]] * 8, axis=1)


def volume_grad_kernel(fs, y_even, y_odd, fg, wt, co, out, co_out, rows_ref, *, c1, nz, ny, nx):
    swap_back = swap_matrix(c1, ny)
    stack_rows(rows_ref, fs, y_even, y_odd)
    for layer in range(nz):
        parts = mm(wt[...], three_layers(rows_ref, slice(None), layer * nx, nx, nx))
        total = fg[:, layer * nx : (layer + 1) * nx] + combine(parts, nx)
        out[:, layer] = mm(swap_back, total.astype(BF16)).reshape(c1, ny, nx).astype(BF16)
    co_out[...] = co[...]


def finish_kernel(*refs, c1, c2, scale_fine, scale_coarse):
    parts, (fine, coarse) = refs[:-2], refs[-2:]
    total = tree_sum([part[...].astype(F32) for part in parts])
    tail = total[9 * c1 :]
    groups = [tail[:c1, r * c1 : (r + 1) * c1] for r in range(8)] + [tail[c1:, :c1]]
    last = jnp.concatenate(groups, axis=0)
    for c in range(3):
        own = slice(c * c1, (c + 1) * c1)
        for ab in range(8):
            fine[ab * 3 + c] = total[own, ab * c1 : (ab + 1) * c1] * scale_fine
        fine[24 + c] = last[own] * scale_fine
    for part, taps in ((total[3 * c1 : 9 * c1], 8), (last[3 * c1 :], 1)):
        turned = part.T * scale_coarse
        for ab in range(taps):
            for c in range(3):
                at = (8 if taps == 1 else ab) * 3 + c
                coarse[at] = turned[ab * c1 : (ab + 1) * c1, c * c2 : (c + 1) * c2]


def tree_sum(values):
    while len(values) > 1:
        values = [values[i] + values[i + 1] for i in range(0, len(values), 2)]
    return values[0]


def shapes(*pairs):
    return [pltpu.VMEM(shape, kind) for shape, kind in pairs]


def result(shape, kind):
    return jax.ShapeDtypeStruct(shape, kind)


def call(body, outs, args, flops=0, scratch=()):
    specs = [pl.BlockSpec(memory_space=pltpu.VMEM) for _ in args]
    nbytes = sum(a.size * a.dtype.itemsize for a in args)
    placed = [pltpu.with_memory_space_constraint(arg, pltpu.VMEM) for arg in args]
    return pl.pallas_call(
        body,
        out_shape=outs,
        in_specs=specs,
        out_specs=[pl.BlockSpec(memory_space=pltpu.VMEM) for _ in outs],
        scratch_shapes=list(scratch),
        compiler_params=pltpu.CompilerParams(vmem_limit_bytes=24 * 2**20),
        cost_estimate=pl.CostEstimate(flops=flops, bytes_accessed=nbytes, transcendentals=0),
    )(*placed)


def swap_pairs(even, odd, axis):
    count = lax.axis_size(axis)
    out = []
    for value, first in ((even, 0), (odd, 1)):
        pairs = [(i, i + 1) for i in range(first, count - 1, 2)]
        pairs += [(target, source) for source, target in pairs]
        out.append(lax.ppermute(value, axis, pairs))
    return out


def swap_bits(value, bits):
    ny = lax.axis_size("gy")
    count = lax.axis_size("gx") * ny
    flip = sum((bit if axis == "gy" else bit * ny) for axis, bit in bits)
    return lax.ppermute(value, ("gx", "gy"), [(i, i ^ flip) for i in range(count)])


def program(volume, fine_kernel, coarse_kernel, fine_cotangent, coarse_cotangent):
    c1, nz, ny, nx = volume.shape
    c2 = coarse_cotangent.shape[0]
    hz, hy, half = nz // 2, ny // 2, nx // 2
    gx, gy = lax.axis_size("gx"), lax.axis_size("gy")
    cells = nz * gx * ny * gy * nx
    sizes = dict(c1=c1, nz=nz, ny=ny, nx=nx)
    rows, half_rows = ny * c1, hy * c1

    own, z_even, z_odd = call(
        volume_rows_kernel,
        shapes(((rows, nz * nx), BF16), ((rows, nx), BF16), ((rows, nx), BF16)),
        [volume],
        flops=10**8,
    )
    z_even, z_odd = swap_pairs(z_even, z_odd, "gx")
    wa, wt, wc, wct = call(
        functools.partial(weights_kernel, ny=ny),
        shapes(
            ((3 * ny * c1, 3 * (ny + 2) * c1), BF16),
            ((3 * ny * c1, 3 * (ny + 2) * c1), BF16),
            ((3 * (hy + 2) * c2, 3 * (hy + 4) * c1), BF16),
            ((3 * hy * c1, 3 * (hy + 2) * c2), BF16),
        ),
        [
            fine_kernel.reshape(27, c1, c1),
            coarse_kernel.swapaxes(3, 4).reshape(27, c1, c2),
        ],
        flops=10**9,
    )
    fine_cot, coarse_cot = call(
        cot_rows_kernel,
        shapes(((rows, nz * nx), BF16), ((hy * c2, hz * half), BF16)),
        [fine_cotangent, coarse_cotangent.reshape(c2, hz * hy, half)],
        flops=10**8,
    )

    layers = (nz + 2) * nx
    stacked = shapes(((rows, layers), BF16), ((c1, layers), BF16), ((c1, layers), BF16))
    own, y_even, y_odd = call(layers_kernel, stacked, [own, z_even, z_odd], flops=10**8)
    y_even, y_odd = swap_pairs(y_even, y_odd, "gy")

    sent = (half_rows, hz * half + 2 * half)
    volume_rows, pre, fine_rows, pooled, z_even, z_odd = call(
        functools.partial(fine_kernel_fn, nz=nz, nx=nx),
        shapes(
            ((rows + 2 * c1, layers), BF16),
            ((rows, nz * nx), F32),
            ((rows, nz * nx), BF16),
            ((half_rows, hz * half), BF16),
            (sent, BF16),
            (sent, BF16),
        ),
        [own, y_even, y_odd, wa, coarse_cot],
        flops=3 * 10**9,
    )
    z_even, z_odd = swap_pairs(z_even, z_odd, "gx")
    fine_out, slopes = call(
        functools.partial(slope_kernel_fn, **sizes),
        [result((c1, nz, ny, nx), BF16)] + shapes(((rows, nz * nx), F32)),
        [pre, fine_rows],
        flops=2 * 10**9,
    )
    pooled_lanes = 3 * hz * half
    cot_lanes = (hz + 2) * half
    sent = (2 * c1, pooled_lanes + cot_lanes)
    pooled, coarse_cot, y_even, y_odd = call(
        coarse_layers_kernel,
        shapes(
            ((half_rows, pooled_lanes), BF16),
            ((hy * c2, cot_lanes), BF16),
            (sent, BF16),
            (sent, BF16),
        ),
        [pooled, coarse_cot, z_even, z_odd],
        flops=10**8,
    )
    y_even, y_odd = swap_pairs(y_even, y_odd, "gy")

    pooled, coarse_slope, coarse_out, fslope, fgrad, z_even, z_odd = call(
        functools.partial(coarse_kernel_fn, c2=c2, **sizes),
        shapes(
            (((hy + 4) * c1, pooled_lanes), BF16),
            (((hy + 2) * c2, cot_lanes), BF16),
            ((c2 * hz * hy, half), BF16),
            ((rows, nz * nx), BF16),
            ((rows, nz * nx), F32),
            ((rows, nx), BF16),
            ((rows, nx), BF16),
        ),
        [pooled, coarse_cot, y_even, y_odd, fine_cot, slopes, wc, wct],
        flops=4 * 10**9,
        scratch=[pltpu.VMEM(((hy + 2) * c2, cot_lanes), BF16)],
    )
    z_even, z_odd = swap_pairs(z_even, z_odd, "gx")
    (terms,) = call(
        functools.partial(terms_kernel, c1=c1, c2=c2, nx=nx),
        shapes(((11 * c1, 8 * c1), F32)),
        [volume_rows, fslope, pooled, coarse_slope],
        flops=2 * 10**9,
    )
    fslope, y_even, y_odd = call(layers_kernel, stacked, [fslope, z_even, z_odd], flops=10**8)
    y_even, y_odd = swap_pairs(y_even, y_odd, "gy")

    bits = [("gy", 1 << n) for n in range(gy.bit_length() - 1)]
    bits += [("gx", 1 << n) for n in range(gx.bit_length() - 1)]
    first = len(bits) % 2
    rounds = [bits[:1]] * first
    rounds += [bits[n : n + 2] for n in range(first, len(bits), 2)]
    value = terms
    for index, group in enumerate(rounds):
        if index:
            value = value.astype(BF16)
        parts = [value]
        for some in [[bit] for bit in group] + [group] * (len(group) == 2):
            parts.append(swap_bits(value, some))
        if index + 1 < len(rounds):
            value = tree_sum([part.astype(F32) for part in parts])
    volume_grad, coarse_out = call(
        functools.partial(volume_grad_kernel, **sizes),
        [result((c1, nz, ny, nx), BF16), result((c2 * hz * hy, half), BF16)],
        [fslope, y_even, y_odd, fgrad, wt, coarse_out],
        flops=2 * 10**9,
        scratch=[pltpu.VMEM((rows + 2 * c1, layers), BF16)],
    )
    fine_grad, coarse_grad = call(
        functools.partial(
            finish_kernel,
            c1=c1,
            c2=c2,
            scale_fine=cells ** (-0.5),
            scale_coarse=(cells // 8) ** (-0.5),
        ),
        [result((27, c1, c1), F32), result((27, c1, c2), F32)],
        parts,
        flops=10**7,
    )
    return (
        fine_out,
        coarse_out.reshape(c2, hz, hy, half),
        volume_grad,
        fine_grad.reshape(fine_kernel.shape),
        coarse_grad.reshape(3, 3, 3, c1, c2).swapaxes(3, 4),
    )


def solution(mesh):
    split = P(None, "gx", "gy", None)
    return jax.shard_map(
        program,
        mesh=mesh,
        in_specs=(split, P(), P(), split, split),
        out_specs=(split, split, split, P(), P()),
        check_vma=False,
    )
```

```python
import functools

import jax
import jax.numpy as jnp
from jax import lax
from jax.experimental import pallas as pl
from jax.experimental.pallas import tpu as pltpu
from jax.sharding import PartitionSpec as P


F32 = jnp.float32
BF16 = jnp.bfloat16


def mm(left, right):
    return jnp.dot(left, right, preferred_element_type=F32)


def mm_t(left, right):
    return lax.dot_general(left, right, (((1,), (1,)), ((), ())), preferred_element_type=F32)


def one_hot(shape, rule):
    rows = lax.broadcasted_iota(jnp.int32, shape, 0)
    cols = lax.broadcasted_iota(jnp.int32, shape, 1)
    return jnp.where(rule(rows, cols), 1.0, 0.0).astype(BF16)


def swap_matrix(outer, inner):
    count = outer * inner
    return one_hot((count, count), lambda r, c: c == (r % inner) * outer + r // inner)


def moved(values, width, offset):
    lanes = values.shape[1]
    place = lax.broadcasted_iota(jnp.int32, values.shape, 1) % width
    if offset == 1:
        return jnp.where(place == 0, 0.0, pltpu.roll(values, 1, 1))
    return jnp.where(place == width - 1, 0.0, pltpu.roll(values, lanes - 1, 1))


def combine(parts, width):
    rows = parts.shape[0] // 3
    return (
        parts[rows : 2 * rows]
        + moved(parts[:rows], width, 1)
        + moved(parts[2 * rows :], width, -1)
    )


def to_rows(values):
    chans, rows, width = values.shape
    return values.astype(F32).reshape(chans * rows, width).astype(BF16)


def band(taps_ref, out_ref, out_rows, turned, flipped):
    m, n = taps_ref.shape[1:][::-1] if turned else taps_ref.shape[1:]
    wide = (out_rows + 2) * n
    spread = one_hot((n, wide), lambda r, c: c % n == r)
    block = lax.broadcasted_iota(jnp.int32, (m, wide), 1) // n
    if turned:
        tiled = [
            lax.dot_general(
                taps_ref[at], spread, (((0,), (0,)), ((), ())), preferred_element_type=F32
            )
            for at in range(27)
        ]
    else:
        every = mm(taps_ref[...].reshape(27 * m, n), spread)
        tiled = [every[at * m : (at + 1) * m] for at in range(27)]
    if flipped:
        tiled = tiled[::-1]
    for a in range(3):
        for c in range(3):
            taps = [tiled[(a * 3 + b) * 3 + c] for b in range(3)]
            for y in range(out_rows):
                value = jnp.where(
                    block == y,
                    taps[0],
                    jnp.where(block == y + 1, taps[1], jnp.where(block == y + 2, taps[2], 0.0)),
                )
                start = (c * out_rows + y) * m
                out_ref[start : start + m, a * wide : (a + 1) * wide] = value.astype(BF16)


def weights_kernel(kf, kc, wa, wt, wc, wct, *, ny):
    band(kf, wa, ny, False, False)
    band(kf, wt, ny, True, True)
    band(kc, wc, ny // 2 + 2, True, False)
    band(kc, wct, ny // 2, False, True)


def ends():
    return [lax.axis_index(axis) % 2 == 0 for axis in ("gx", "gy")]


def from_odd(value, axis):
    at = lax.axis_index(axis)
    alone = jnp.logical_or(at == 0, at == lax.axis_size(axis) - 1)
    return jnp.where(alone, jnp.zeros_like(value), value)


def volume_rows_kernel(vol, own, even, odd):
    c1, nz, ny, nx = vol.shape
    swap = swap_matrix(ny, c1)
    for z in range(nz):
        own[:, z * nx : (z + 1) * nx] = mm(swap, to_rows(vol[:, z])).astype(BF16)
    low, high = own[:, : even.shape[1]], own[:, own.shape[1] - even.shape[1] :]
    first = ends()[0]
    even[...] = jnp.where(first, high, low)
    odd[...] = jnp.where(first, low, high)


def cot_rows_kernel(fc, cc, fine, coarse):
    c1, nz, ny, nx = fc.shape
    c2, cells, half = cc.shape
    hy = ny // 2
    swap = swap_matrix(ny, c1)
    for z in range(nz):
        fine[:, z * nx : (z + 1) * nx] = mm(swap, to_rows(fc[:, z])).astype(BF16)
    rows = mm(swap_matrix(cells, c2), to_rows(cc[...])).astype(BF16)
    for z in range(cells // hy):
        coarse[:, z * half : (z + 1) * half] = rows[z * hy * c2 : (z + 1) * hy * c2]


def stack_layers(out, own, even, odd):
    first = ends()[0]
    width = even.shape[1]
    low, high = even[...], from_odd(odd[...], "gx")
    out[:, :width] = jnp.where(first, high, low)
    out[:, width : width + own.shape[1]] = own[...]
    out[:, width + own.shape[1] :] = jnp.where(first, low, high)


def stack_rows(out, own, even, odd):
    first = ends()[1]
    edge = even.shape[0]
    low, high = even[...], from_odd(odd[...], "gy")
    out[:edge] = jnp.where(first, high, low)
    out[edge : edge + own.shape[0]] = own[...]
    out[edge + own.shape[0] :] = jnp.where(first, low, high)


def layers_kernel(own, z_even, z_odd, out, even, odd):
    stack_layers(out, own, z_even, z_odd)
    edge = even.shape[0]
    first = ends()[1]
    low, high = out[:edge], out[out.shape[0] - edge :]
    even[...] = jnp.where(first, high, low)
    odd[...] = jnp.where(first, low, high)


def coarse_layers_kernel(po, co, z_even, z_odd, p_out, c_out, even, odd):
    lanes, rows = po.shape[1], po.shape[0]
    half = (z_even.shape[1] - lanes) // 2
    stack_layers(p_out, po, z_even.at[:, :lanes], z_odd.at[:, :lanes])
    first = ends()[0]
    width = co.shape[1]
    for part in range(2):
        span = slice(lanes + part * half, lanes + (part + 1) * half)
        low, high = z_even[:, span], from_odd(z_odd[:, span], "gx")
        into = slice(part * rows, (part + 1) * rows)
        c_out[into, :half] = jnp.where(first, high, low)
        c_out[into, half + width :] = jnp.where(first, low, high)
    c_out[:, half : half + width] = co[...]
    edge = even.shape[0]
    pooled = p_out.shape[1]
    first = ends()[1]
    for ref, span in ((p_out, slice(0, pooled)), (c_out, slice(pooled, even.shape[1]))):
        low, high = ref[:edge], ref[ref.shape[0] - edge :]
        even[:, span] = jnp.where(first, high, low)
        odd[:, span] = jnp.where(first, low, high)


def three_layers(ref, rows, first, step, width):
    return jnp.concatenate(
        [ref[rows, first + dz * step : first + dz * step + width] for dz in range(3)], axis=0
    )


def fine_kernel_fn(xo, y_even, y_odd, wa, co, x_ref, pre_out, fo_out, po, z_even, z_odd, *, nz, nx):
    c1 = y_even.shape[0]
    half = nx // 2
    stack_rows(x_ref, xo, y_even, y_odd)
    pool = one_hot((nx, half), lambda r, c: r // 2 == c)
    rows = xo.shape[0]
    for layer in range(nz):
        parts = mm(wa[...], three_layers(x_ref, slice(None), layer * nx, nx, nx))
        pre = combine(parts, nx)
        pre_out[:, layer * nx : (layer + 1) * nx] = pre
        value = xo[:, (layer + 1) * nx : (layer + 2) * nx].astype(F32)
        fo = (value + pre * jax.nn.sigmoid(pre)).astype(BF16)
        fo_out[:, layer * nx : (layer + 1) * nx] = fo
        pooled = mm(fo, pool)
        if layer % 2 == 0:
            sums = pooled
            continue
        sums = sums + pooled
        cells = [
            sums[2 * r * c1 : (2 * r + 1) * c1] + sums[(2 * r + 1) * c1 : (2 * r + 2) * c1]
            for r in range(rows // c1 // 2)
        ]
        place = layer // 2
        value = jnp.concatenate(cells, axis=0) * 0.125
        po[:, place * half : (place + 1) * half] = value.astype(BF16)
    lanes = po.shape[1]
    low, high = co[:, :half], co[:, co.shape[1] - half :]
    first = ends()[0]
    for ref, value in (
        (z_even, jnp.where(first, high, low)),
        (z_odd, jnp.where(first, low, high)),
    ):
        ref[:, :lanes] = po[...]
        ref[:, lanes : lanes + half] = value[: rows // 2]
        ref[:, lanes + half :] = value[rows // 2 :]


def slope_kernel_fn(pre_ref, fo, fo_out, sl_out, *, c1, nz, ny, nx):
    swap_back = swap_matrix(c1, ny)
    for layer in range(nz):
        span = slice(layer * nx, (layer + 1) * nx)
        pre = pre_ref[:, span]
        sig = jax.nn.sigmoid(pre)
        sl_out[:, span] = sig * (1.0 + pre * (1.0 - sig))
        rows = mm(swap_back, fo[:, span])
        fo_out[:, layer] = rows.reshape(c1, ny, nx).astype(BF16)


def coarse_kernel_fn(
    po, cc, y_even, y_odd, fc, sl, wc, wct,
    p_ref, cs_ref, co_out, fs_out, fg_out, z_even, z_odd, c_ref, *, c1, c2, nz, ny, nx,
):
    half, hz, hy = nx // 2, nz // 2, ny // 2
    pooled = po.shape[1]
    stack_rows(p_ref, po, y_even.at[:, :pooled], y_odd.at[:, :pooled])
    stack_rows(c_ref, cc, y_even.at[:, pooled:], y_odd.at[:, pooled:])
    inner = slice(c2, c2 + hy * c2)
    own = []
    for pair in range((hz + 2) // 2):
        pre = combine(mm(wc[...], three_layers(p_ref, slice(None), pair * nx, half, nx)), half)
        sig = jax.nn.sigmoid(pre)
        span = slice(pair * nx, (pair + 1) * nx)
        cot = c_ref[:, span].astype(F32)
        cs_ref[:, span] = (cot * (sig * (1.0 + pre * (1.0 - sig)))).astype(BF16)
        out = (pre[inner] * sig[inner]).astype(BF16)
        own += [out[:, :half], out[:, half:]]
    stacked = jnp.concatenate(own[1:-1], axis=0)
    co_out[...] = mm(swap_matrix(c2, hz * hy), stacked).astype(BF16)
    widen = one_hot((half, nx), lambda r, c: c // 2 == r)
    for pair in range(hz // 2):
        parts = mm(wct[...], three_layers(cs_ref, slice(None), pair * nx, half, nx))
        grad = combine(parts, half) * 0.125
        high = grad.astype(BF16)
        low = (grad - high.astype(F32)).astype(BF16)
        for side in range(2):
            lanes = slice(side * half, (side + 1) * half)
            up = mm(high[:, lanes], widen) + mm(low[:, lanes], widen)
            blocks = [up[y // 2 * c1 : y // 2 * c1 + c1] for y in range(ny)]
            spread = jnp.concatenate(blocks, axis=0)
            for layer in (4 * pair + 2 * side, 4 * pair + 2 * side + 1):
                span = slice(layer * nx, (layer + 1) * nx)
                total = fc[:, span].astype(F32) + spread
                fg_out[:, span] = total
                fs_out[:, span] = (total * sl[:, span]).astype(BF16)
    low, high = fs_out[:, :nx], fs_out[:, (nz - 1) * nx :]
    first = ends()[0]
    z_even[...] = jnp.where(first, high, low)
    z_odd[...] = jnp.where(first, low, high)


def terms_of(slopes, cells, chans, count, width, rows, lanes):
    slopes = slopes.astype(F32)
    shifted = [moved(slopes, width, -1), slopes, moved(slopes, width, 1)]
    shifted = [value.astype(BF16) for value in shifted]
    total = None
    for y in range(slopes.shape[0] // chans):
        left = jnp.concatenate([s[y * chans : (y + 1) * chans] for s in shifted], axis=0)
        first = y * count + rows
        right = [
            cells[first : first + 3 * count, lanes + a * width : lanes + a * width + slopes.shape[1]]
            for a in range(3)
        ]
        term = mm_t(left, jnp.concatenate(right, axis=0))
        total = term if total is None else total + term
    return total


def terms_kernel(x_ref, fs, p_ref, cs, g_out, *, c1, c2, nx):
    half = nx // 2
    fine = terms_of(fs[...], x_ref, c1, c1, nx, 0, 0)
    inner = cs[c2 : cs.shape[0] - c2, half : cs.shape[1] - half]
    coarse = terms_of(inner, p_ref, c2, c1, half, c1, half)
    three = 3 * c1
    g_out[:three, :] = fine[:, : 8 * c1]
    g_out[three : 9 * c1, :] = coarse[:, : 8 * c1]
    last = jnp.concatenate([fine[:, 8 * c1 :], coarse[:, 8 * c1 :]], axis=0)
    groups = [last[r * c1 : (r + 1) * c1] for r in range(9)]
    g_out[9 * c1 : 10 * c1, :] = jnp.concatenate(groups[:8], axis=1)
    g_out[10 * c1 :, :] = jnp.concatenate([groups[8]] * 8, axis=1)


def volume_grad_kernel(fs, y_even, y_odd, fg, wt, co, out, co_out, rows_ref, *, c1, nz, ny, nx):
    swap_back = swap_matrix(c1, ny)
    stack_rows(rows_ref, fs, y_even, y_odd)
    for layer in range(nz):
        parts = mm(wt[...], three_layers(rows_ref, slice(None), layer * nx, nx, nx))
        total = fg[:, layer * nx : (layer + 1) * nx] + combine(parts, nx)
        out[:, layer] = mm(swap_back, total.astype(BF16)).reshape(c1, ny, nx).astype(BF16)
    co_out[...] = co[...]


def finish_kernel(*refs, c1, c2, scale_fine, scale_coarse):
    parts, (fine, coarse) = refs[:-2], refs[-2:]
    total = tree_sum([part[...].astype(F32) for part in parts])
    tail = total[9 * c1 :]
    groups = [tail[:c1, r * c1 : (r + 1) * c1] for r in range(8)] + [tail[c1:, :c1]]
    last = jnp.concatenate(groups, axis=0)
    for c in range(3):
        own = slice(c * c1, (c + 1) * c1)
        for ab in range(8):
            fine[ab * 3 + c] = total[own, ab * c1 : (ab + 1) * c1] * scale_fine
        fine[24 + c] = last[own] * scale_fine
    for part, taps in ((total[3 * c1 : 9 * c1], 8), (last[3 * c1 :], 1)):
        turned = part.T * scale_coarse
        for ab in range(taps):
            for c in range(3):
                at = (8 if taps == 1 else ab) * 3 + c
                coarse[at] = turned[ab * c1 : (ab + 1) * c1, c * c2 : (c + 1) * c2]


def tree_sum(values):
    while len(values) > 1:
        values = [values[i] + values[i + 1] for i in range(0, len(values), 2)]
    return values[0]


def shapes(*pairs):
    return [pltpu.VMEM(shape, kind) for shape, kind in pairs]


def result(shape, kind):
    return jax.ShapeDtypeStruct(shape, kind)


def call(body, outs, args, flops=0, scratch=()):
    specs = [pl.BlockSpec(memory_space=pltpu.VMEM) for _ in args]
    nbytes = sum(a.size * a.dtype.itemsize for a in args)
    placed = [pltpu.with_memory_space_constraint(arg, pltpu.VMEM) for arg in args]
    return pl.pallas_call(
        body,
        out_shape=outs,
        in_specs=specs,
        out_specs=[pl.BlockSpec(memory_space=pltpu.VMEM) for _ in outs],
        scratch_shapes=list(scratch),
        compiler_params=pltpu.CompilerParams(vmem_limit_bytes=24 * 2**20),
        cost_estimate=pl.CostEstimate(flops=flops, bytes_accessed=nbytes, transcendentals=0),
    )(*placed)


def swap_pairs(even, odd, axis):
    nx, ny = lax.axis_size("gx"), lax.axis_size("gy")
    out = []
    for value, first in ((even, 0), (odd, 1)):
        pairs = []
        for place in range(nx * ny):
            at = [place // ny, place % ny]
            own = 0 if axis == "gx" else 1
            if first and at[own] in (0, (nx, ny)[own] - 1):
                at[1 - own] ^= 1
            else:
                at[own] = ((at[own] + first) ^ 1) - first
            pairs.append((place, at[0] * ny + at[1]))
        out.append(lax.ppermute(value, ("gx", "gy"), pairs))
    return out


def swap_bits(value, bits):
    ny = lax.axis_size("gy")
    count = lax.axis_size("gx") * ny
    flip = sum((bit if axis == "gy" else bit * ny) for axis, bit in bits)
    return lax.ppermute(value, ("gx", "gy"), [(i, i ^ flip) for i in range(count)])


def program(volume, fine_kernel, coarse_kernel, fine_cotangent, coarse_cotangent):
    c1, nz, ny, nx = volume.shape
    c2 = coarse_cotangent.shape[0]
    hz, hy, half = nz // 2, ny // 2, nx // 2
    gx, gy = lax.axis_size("gx"), lax.axis_size("gy")
    cells = nz * gx * ny * gy * nx
    sizes = dict(c1=c1, nz=nz, ny=ny, nx=nx)
    rows, half_rows = ny * c1, hy * c1

    own, z_even, z_odd = call(
        volume_rows_kernel,
        shapes(((rows, nz * nx), BF16), ((rows, nx), BF16), ((rows, nx), BF16)),
        [volume],
        flops=10**8,
    )
    z_even, z_odd = swap_pairs(z_even, z_odd, "gx")
    wa, wt, wc, wct = call(
        functools.partial(weights_kernel, ny=ny),
        shapes(
            ((3 * ny * c1, 3 * (ny + 2) * c1), BF16),
            ((3 * ny * c1, 3 * (ny + 2) * c1), BF16),
            ((3 * (hy + 2) * c2, 3 * (hy + 4) * c1), BF16),
            ((3 * hy * c1, 3 * (hy + 2) * c2), BF16),
        ),
        [
            fine_kernel.reshape(27, c1, c1),
            coarse_kernel.swapaxes(3, 4).reshape(27, c1, c2),
        ],
        flops=10**9,
    )
    fine_cot, coarse_cot = call(
        cot_rows_kernel,
        shapes(((rows, nz * nx), BF16), ((hy * c2, hz * half), BF16)),
        [fine_cotangent, coarse_cotangent.reshape(c2, hz * hy, half)],
        flops=10**8,
    )

    layers = (nz + 2) * nx
    stacked = shapes(((rows, layers), BF16), ((c1, layers), BF16), ((c1, layers), BF16))
    own, y_even, y_odd = call(layers_kernel, stacked, [own, z_even, z_odd], flops=10**8)
    y_even, y_odd = swap_pairs(y_even, y_odd, "gy")

    sent = (half_rows, hz * half + 2 * half)
    volume_rows, pre, fine_rows, pooled, z_even, z_odd = call(
        functools.partial(fine_kernel_fn, nz=nz, nx=nx),
        shapes(
            ((rows + 2 * c1, layers), BF16),
            ((rows, nz * nx), F32),
            ((rows, nz * nx), BF16),
            ((half_rows, hz * half), BF16),
            (sent, BF16),
            (sent, BF16),
        ),
        [own, y_even, y_odd, wa, coarse_cot],
        flops=3 * 10**9,
    )
    z_even, z_odd = swap_pairs(z_even, z_odd, "gx")
    fine_out, slopes = call(
        functools.partial(slope_kernel_fn, **sizes),
        [result((c1, nz, ny, nx), BF16)] + shapes(((rows, nz * nx), F32)),
        [pre, fine_rows],
        flops=2 * 10**9,
    )
    pooled_lanes = 3 * hz * half
    cot_lanes = (hz + 2) * half
    sent = (2 * c1, pooled_lanes + cot_lanes)
    pooled, coarse_cot, y_even, y_odd = call(
        coarse_layers_kernel,
        shapes(
            ((half_rows, pooled_lanes), BF16),
            ((hy * c2, cot_lanes), BF16),
            (sent, BF16),
            (sent, BF16),
        ),
        [pooled, coarse_cot, z_even, z_odd],
        flops=10**8,
    )
    y_even, y_odd = swap_pairs(y_even, y_odd, "gy")

    pooled, coarse_slope, coarse_out, fslope, fgrad, z_even, z_odd = call(
        functools.partial(coarse_kernel_fn, c2=c2, **sizes),
        shapes(
            (((hy + 4) * c1, pooled_lanes), BF16),
            (((hy + 2) * c2, cot_lanes), BF16),
            ((c2 * hz * hy, half), BF16),
            ((rows, nz * nx), BF16),
            ((rows, nz * nx), F32),
            ((rows, nx), BF16),
            ((rows, nx), BF16),
        ),
        [pooled, coarse_cot, y_even, y_odd, fine_cot, slopes, wc, wct],
        flops=4 * 10**9,
        scratch=[pltpu.VMEM(((hy + 2) * c2, cot_lanes), BF16)],
    )
    z_even, z_odd = swap_pairs(z_even, z_odd, "gx")
    (terms,) = call(
        functools.partial(terms_kernel, c1=c1, c2=c2, nx=nx),
        shapes(((11 * c1, 8 * c1), F32)),
        [volume_rows, fslope, pooled, coarse_slope],
        flops=2 * 10**9,
    )
    fslope, y_even, y_odd = call(layers_kernel, stacked, [fslope, z_even, z_odd], flops=10**8)
    y_even, y_odd = swap_pairs(y_even, y_odd, "gy")

    bits = [("gy", 1 << n) for n in range(gy.bit_length() - 1)]
    bits += [("gx", 1 << n) for n in range(gx.bit_length() - 1)]
    first = len(bits) % 2
    rounds = [bits[:1]] * first
    rounds += [bits[n : n + 2] for n in range(first, len(bits), 2)]
    value = terms
    for index, group in enumerate(rounds):
        if index:
            value = value.astype(BF16)
        parts = [value]
        for some in [[bit] for bit in group] + [group] * (len(group) == 2):
            parts.append(swap_bits(value, some))
        if index + 1 < len(rounds):
            value = tree_sum([part.astype(F32) for part in parts])
    volume_grad, coarse_out = call(
        functools.partial(volume_grad_kernel, **sizes),
        [result((c1, nz, ny, nx), BF16), result((c2 * hz * hy, half), BF16)],
        [fslope, y_even, y_odd, fgrad, wt, coarse_out],
        flops=2 * 10**9,
        scratch=[pltpu.VMEM((rows + 2 * c1, layers), BF16)],
    )
    fine_grad, coarse_grad = call(
        functools.partial(
            finish_kernel,
            c1=c1,
            c2=c2,
            scale_fine=cells ** (-0.5),
            scale_coarse=(cells // 8) ** (-0.5),
        ),
        [result((27, c1, c1), F32), result((27, c1, c2), F32)],
        parts,
        flops=10**7,
    )
    return (
        fine_out,
        coarse_out.reshape(c2, hz, hy, half),
        volume_grad,
        fine_grad.reshape(fine_kernel.shape),
        coarse_grad.reshape(3, 3, 3, c1, c2).swapaxes(3, 4),
    )


def solution(mesh):
    split = P(None, "gx", "gy", None)
    return jax.shard_map(
        program,
        mesh=mesh,
        in_specs=(split, P(), P(), split, split),
        out_specs=(split, split, split, P(), P()),
        check_vma=False,
    )
```

```python
import functools

import jax
import jax.numpy as jnp
from jax import lax
from jax.experimental import pallas as pl
from jax.experimental.pallas import tpu as pltpu
from jax.sharding import PartitionSpec as P


F32 = jnp.float32
BF16 = jnp.bfloat16


def mm(left, right):
    return jnp.dot(left, right, preferred_element_type=F32)


def mm_t(left, right):
    return lax.dot_general(left, right, (((1,), (1,)), ((), ())), preferred_element_type=F32)


def one_hot(shape, rule):
    rows = lax.broadcasted_iota(jnp.int32, shape, 0)
    cols = lax.broadcasted_iota(jnp.int32, shape, 1)
    return jnp.where(rule(rows, cols), 1.0, 0.0).astype(BF16)


def swap_matrix(outer, inner):
    count = outer * inner
    return one_hot((count, count), lambda r, c: c == (r % inner) * outer + r // inner)


def moved(values, width, offset):
    lanes = values.shape[1]
    place = lax.broadcasted_iota(jnp.int32, values.shape, 1) % width
    if offset == 1:
        return jnp.where(place == 0, 0.0, pltpu.roll(values, 1, 1))
    return jnp.where(place == width - 1, 0.0, pltpu.roll(values, lanes - 1, 1))


def combine(parts, width):
    rows = parts.shape[0] // 3
    return (
        parts[rows : 2 * rows]
        + moved(parts[:rows], width, 1)
        + moved(parts[2 * rows :], width, -1)
    )


def to_rows(values):
    chans, rows, width = values.shape
    return values.astype(F32).reshape(chans * rows, width).astype(BF16)


def band(taps_ref, out_ref, out_rows, in_rows, shift, turned, flipped):
    m, n = taps_ref.shape[1:][::-1] if turned else taps_ref.shape[1:]
    wide = in_rows * n
    spread = one_hot((n, wide), lambda r, c: c % n == r)
    block = lax.broadcasted_iota(jnp.int32, (m, wide), 1) // n
    if turned:
        tiled = [
            lax.dot_general(
                taps_ref[at], spread, (((0,), (0,)), ((), ())), preferred_element_type=F32
            )
            for at in range(27)
        ]
    else:
        every = mm(taps_ref[...].reshape(27 * m, n), spread)
        tiled = [every[at * m : (at + 1) * m] for at in range(27)]
    if flipped:
        tiled = tiled[::-1]
    for a in range(3):
        for c in range(3):
            taps = [tiled[(a * 3 + b) * 3 + c] for b in range(3)]
            for y in range(out_rows):
                value = jnp.zeros((m, wide), F32)
                for b in range(3):
                    if 0 <= y + b - shift < in_rows:
                        value = jnp.where(block == y + b - shift, taps[b], value)
                start = (c * out_rows + y) * m
                out_ref[start : start + m, a * wide : (a + 1) * wide] = value.astype(BF16)


def weights_kernel(kf, kc, wa, wl, wh, wt, wc, wcl, wch, wct, *, ny):
    hy = ny // 2
    band(kf, wa, ny, ny, 1, False, False)
    band(kf, wl, 1, 1, 0, False, False)
    band(kf, wh, 1, 1, 2, False, False)
    band(kc, wc, hy + 2, hy, 2, True, False)
    band(kc, wcl, 2, 2, 0, True, False)
    band(kc, wch, 2, 2, 2, True, False)
    band(kf, wt, ny, ny + 2, 0, True, True)
    band(kc, wct, hy, hy + 2, 0, False, True)


def ends():
    return [lax.axis_index(axis) % 2 == 0 for axis in ("gx", "gy")]


def from_odd(value, axis):
    at = lax.axis_index(axis)
    alone = jnp.logical_or(at == 0, at == lax.axis_size(axis) - 1)
    return jnp.where(alone, jnp.zeros_like(value), value)


def volume_rows_kernel(vol, own, even, odd):
    c1, nz, ny, nx = vol.shape
    swap = swap_matrix(ny, c1)
    for z in range(nz):
        own[:, z * nx : (z + 1) * nx] = mm(swap, to_rows(vol[:, z])).astype(BF16)
    low, high = own[:, : even.shape[1]], own[:, own.shape[1] - even.shape[1] :]
    first = ends()[0]
    even[...] = jnp.where(first, high, low)
    odd[...] = jnp.where(first, low, high)


def cot_rows_kernel(fc, cc, fine, coarse):
    c1, nz, ny, nx = fc.shape
    c2, cells, half = cc.shape
    hy = ny // 2
    swap = swap_matrix(ny, c1)
    for z in range(nz):
        fine[:, z * nx : (z + 1) * nx] = mm(swap, to_rows(fc[:, z])).astype(BF16)
    rows = mm(swap_matrix(cells, c2), to_rows(cc[...])).astype(BF16)
    for z in range(cells // hy):
        coarse[:, z * half : (z + 1) * half] = rows[z * hy * c2 : (z + 1) * hy * c2]


def stack_layers(out, own, even, odd):
    first = ends()[0]
    width = even.shape[1]
    low, high = even[...], from_odd(odd[...], "gx")
    out[:, :width] = jnp.where(first, high, low)
    out[:, width : width + own.shape[1]] = own[...]
    out[:, width + own.shape[1] :] = jnp.where(first, low, high)


def stack_rows(out, own, even, odd):
    first = ends()[1]
    edge = even.shape[0]
    low, high = even[...], from_odd(odd[...], "gy")
    out[:edge] = jnp.where(first, high, low)
    out[edge : edge + own.shape[0]] = own[...]
    out[edge + own.shape[0] :] = jnp.where(first, low, high)


def layers_kernel(own, z_even, z_odd, out, even, odd):
    stack_layers(out, own, z_even, z_odd)
    edge = even.shape[0]
    first = ends()[1]
    low, high = out[:edge], out[out.shape[0] - edge :]
    even[...] = jnp.where(first, high, low)
    odd[...] = jnp.where(first, low, high)


def coarse_layers_kernel(po, co, z_even, z_odd, p_out, c_out, even, odd):
    lanes, rows = po.shape[1], po.shape[0]
    half = (z_even.shape[1] - lanes) // 2
    stack_layers(p_out, po, z_even.at[:, :lanes], z_odd.at[:, :lanes])
    first = ends()[0]
    width = co.shape[1]
    for part in range(2):
        span = slice(lanes + part * half, lanes + (part + 1) * half)
        low, high = z_even[:, span], from_odd(z_odd[:, span], "gx")
        into = slice(part * rows, (part + 1) * rows)
        c_out[into, :half] = jnp.where(first, high, low)
        c_out[into, half + width :] = jnp.where(first, low, high)
    c_out[:, half : half + width] = co[...]
    edge = even.shape[0]
    pooled = p_out.shape[1]
    first = ends()[1]
    for ref, span in ((p_out, slice(0, pooled)), (c_out, slice(pooled, even.shape[1]))):
        low, high = ref[:edge], ref[ref.shape[0] - edge :]
        even[:, span] = jnp.where(first, high, low)
        odd[:, span] = jnp.where(first, low, high)


def three_layers(ref, rows, first, step, width):
    return jnp.concatenate(
        [ref[rows, first + dz * step : first + dz * step + width] for dz in range(3)], axis=0
    )


def neighbours(even, odd, axis):
    first = ends()[0 if axis == "gx" else 1]
    odd = from_odd(odd, axis)
    return jnp.where(first, odd, even), jnp.where(first, even, odd)


def all_layers(values, count, step):
    return jnp.concatenate([values[:, dz * step : (dz + count) * step] for dz in range(3)], axis=0)


def fine_inner_kernel(xo, wa, pre_out, fo_out, sums_out, *, c1, nz, nx):
    half = nx // 2
    pool = one_hot((nx, half), lambda r, c: r // 2 == c)
    inner = slice(c1, xo.shape[0] - c1)
    for layer in range(nz):
        pre = combine(mm(wa[...], three_layers(xo, slice(None), layer * nx, nx, nx)), nx)
        span = slice(layer * nx, (layer + 1) * nx)
        pre_out[:, span] = pre
        pre = pre[inner]
        value = xo[inner, (layer + 1) * nx : (layer + 2) * nx].astype(F32)
        fo = (value + pre * jax.nn.sigmoid(pre)).astype(BF16)
        fo_out[:, span] = fo
        pooled = mm(fo, pool)
        sums = pooled if layer % 2 == 0 else sums + pooled
        if layer % 2:
            sums_out[:, layer // 2 * half : (layer // 2 + 1) * half] = sums


def fine_edge_kernel(
    xo, y_even, y_odd, wl, wh, pre_ref, sums, co, pre_out, fo_out, po, z_even, z_odd, *, nz, nx
):
    c1 = y_even.shape[0]
    half = nx // 2
    rows = xo.shape[0]
    low, high = neighbours(y_even[...], y_odd[...], "gy")
    last = slice(rows - c1, rows)
    pre = jnp.concatenate(
        [
            pre_ref[:c1] + combine(mm(wl[...], all_layers(low, nz, nx)), nx),
            pre_ref[last] + combine(mm(wh[...], all_layers(high, nz, nx)), nx),
        ],
        axis=0,
    )
    pre_out[...] = pre
    own = slice(nx, (nz + 1) * nx)
    value = jnp.concatenate([xo[:c1, own], xo[last, own]], axis=0).astype(F32)
    fo = (value + pre * jax.nn.sigmoid(pre)).astype(BF16)
    fo_out[...] = fo
    pool = one_hot((nx, half), lambda r, c: r // 2 == c)
    for place in range(nz // 2):
        first = 2 * place * nx
        pooled = mm(fo[:, first : first + nx], pool) + mm(fo[:, first + nx : first + 2 * nx], pool)
        span = slice(place * half, (place + 1) * half)
        cells = [pooled[:c1]] + [sums[r * c1 : (r + 1) * c1, span] for r in range(rows // c1 - 2)]
        cells.append(pooled[c1:])
        cells = [cells[r] + cells[r + 1] for r in range(0, len(cells), 2)]
        po[:, span] = (jnp.concatenate(cells, axis=0) * 0.125).astype(BF16)
    lanes = po.shape[1]
    low, high = co[:, :half], co[:, co.shape[1] - half :]
    first = ends()[0]
    for ref, value in (
        (z_even, jnp.where(first, high, low)),
        (z_odd, jnp.where(first, low, high)),
    ):
        ref[:, :lanes] = po[...]
        ref[:, lanes : lanes + half] = value[: rows // 2]
        ref[:, lanes + half :] = value[rows // 2 :]


def slope_kernel_fn(
    xo, y_even, y_odd, pre_ref, pre_edge, fo, fo_edge, fo_out, sl_out, x_ref, *, c1, nz, ny, nx
):
    stack_rows(x_ref, xo, y_even, y_odd)
    swap_back = swap_matrix(c1, ny)
    for layer in range(nz):
        span = slice(layer * nx, (layer + 1) * nx)
        pre = jnp.concatenate(
            [pre_edge[:c1, span], pre_ref[c1 : c1 * (ny - 1), span], pre_edge[c1:, span]], axis=0
        )
        sig = jax.nn.sigmoid(pre)
        sl_out[:, span] = sig * (1.0 + pre * (1.0 - sig))
        rows = jnp.concatenate([fo_edge[:c1, span], fo[:, span], fo_edge[c1:, span]], axis=0)
        fo_out[:, layer] = mm(swap_back, rows).reshape(c1, ny, nx).astype(BF16)


def coarse_inner_kernel(po, wc, pre_out, *, count, half):
    for pair in range(count // 2):
        parts = mm(wc[...], three_layers(po, slice(None), pair * 2 * half, half, 2 * half))
        pre_out[:, pair * 2 * half : (pair + 1) * 2 * half] = combine(parts, half)


def coarse_kernel_fn(
    po, cc, y_even, y_odd, fc, sl, pre_ref, wcl, wch, wct,
    p_ref, cs_ref, co_out, fs_out, fg_out, z_even, z_odd, *, c1, c2, nz, ny, nx,
):
    half, hz, hy = nx // 2, nz // 2, ny // 2
    pooled = po.shape[1]
    low, high = neighbours(y_even[...], y_odd[...], "gy")
    edge = low.shape[0]
    p_ref[:edge] = low[:, :pooled]
    p_ref[edge : edge + po.shape[0]] = po[...]
    p_ref[edge + po.shape[0] :] = high[:, :pooled]
    count = hz + 2
    pre = jnp.concatenate(
        [
            combine(mm(wcl[...], all_layers(low[:, :pooled], count, half)), half),
            jnp.zeros(((hy - 2) * c2, count * half), F32),
            combine(mm(wch[...], all_layers(high[:, :pooled], count, half)), half),
        ],
        axis=0,
    )
    pre = pre + pre_ref[...]
    sig = jax.nn.sigmoid(pre)
    cot = jnp.concatenate([low[:, pooled:], cc[...], high[:, pooled:]], axis=0).astype(F32)
    cs_ref[...] = (cot * (sig * (1.0 + pre * (1.0 - sig)))).astype(BF16)
    inner = slice(c2, c2 + hy * c2)
    out = (pre[inner, half:-half] * sig[inner, half:-half]).astype(BF16)
    stacked = jnp.concatenate([out[:, z * half : (z + 1) * half] for z in range(hz)], axis=0)
    co_out[...] = mm(swap_matrix(c2, hz * hy), stacked).astype(BF16)
    widen = one_hot((half, nx), lambda r, c: c // 2 == r)
    for pair in range(hz // 2):
        parts = mm(wct[...], three_layers(cs_ref, slice(None), pair * nx, half, nx))
        grad = combine(parts, half) * 0.125
        high = grad.astype(BF16)
        low = (grad - high.astype(F32)).astype(BF16)
        for side in range(2):
            lanes = slice(side * half, (side + 1) * half)
            up = mm(high[:, lanes], widen) + mm(low[:, lanes], widen)
            blocks = [up[y // 2 * c1 : y // 2 * c1 + c1] for y in range(ny)]
            spread = jnp.concatenate(blocks, axis=0)
            for layer in (4 * pair + 2 * side, 4 * pair + 2 * side + 1):
                span = slice(layer * nx, (layer + 1) * nx)
                total = fc[:, span].astype(F32) + spread
                fg_out[:, span] = total
                fs_out[:, span] = (total * sl[:, span]).astype(BF16)
    low, high = fs_out[:, :nx], fs_out[:, (nz - 1) * nx :]
    first = ends()[0]
    z_even[...] = jnp.where(first, high, low)
    z_odd[...] = jnp.where(first, low, high)


def terms_of(slopes, cells, chans, count, width, rows, lanes):
    slopes = slopes.astype(F32)
    shifted = [moved(slopes, width, -1), slopes, moved(slopes, width, 1)]
    shifted = [value.astype(BF16) for value in shifted]
    total = None
    for y in range(slopes.shape[0] // chans):
        left = jnp.concatenate([s[y * chans : (y + 1) * chans] for s in shifted], axis=0)
        first = y * count + rows
        right = [
            cells[first : first + 3 * count, lanes + a * width : lanes + a * width + slopes.shape[1]]
            for a in range(3)
        ]
        term = mm_t(left, jnp.concatenate(right, axis=0))
        total = term if total is None else total + term
    return total


def terms_kernel(x_ref, fs, p_ref, cs, g_out, *, c1, c2, nx):
    half = nx // 2
    fine = terms_of(fs[...], x_ref, c1, c1, nx, 0, 0)
    inner = cs[c2 : cs.shape[0] - c2, half : cs.shape[1] - half]
    coarse = terms_of(inner, p_ref, c2, c1, half, c1, half)
    three = 3 * c1
    g_out[:three, :] = fine[:, : 8 * c1]
    g_out[three : 9 * c1, :] = coarse[:, : 8 * c1]
    last = jnp.concatenate([fine[:, 8 * c1 :], coarse[:, 8 * c1 :]], axis=0)
    groups = [last[r * c1 : (r + 1) * c1] for r in range(9)]
    g_out[9 * c1 : 10 * c1, :] = jnp.concatenate(groups[:8], axis=1)
    g_out[10 * c1 :, :] = jnp.concatenate([groups[8]] * 8, axis=1)


def volume_grad_kernel(fs, y_even, y_odd, fg, wt, co, out, co_out, rows_ref, *, c1, nz, ny, nx):
    swap_back = swap_matrix(c1, ny)
    stack_rows(rows_ref, fs, y_even, y_odd)
    for layer in range(nz):
        parts = mm(wt[...], three_layers(rows_ref, slice(None), layer * nx, nx, nx))
        total = fg[:, layer * nx : (layer + 1) * nx] + combine(parts, nx)
        out[:, layer] = mm(swap_back, total.astype(BF16)).reshape(c1, ny, nx).astype(BF16)
    co_out[...] = co[...]


def finish_kernel(*refs, c1, c2, scale_fine, scale_coarse):
    parts, (fine, coarse) = refs[:-2], refs[-2:]
    total = tree_sum([part[...].astype(F32) for part in parts])
    tail = total[9 * c1 :]
    groups = [tail[:c1, r * c1 : (r + 1) * c1] for r in range(8)] + [tail[c1:, :c1]]
    last = jnp.concatenate(groups, axis=0)
    for c in range(3):
        own = slice(c * c1, (c + 1) * c1)
        for ab in range(8):
            fine[ab * 3 + c] = total[own, ab * c1 : (ab + 1) * c1] * scale_fine
        fine[24 + c] = last[own] * scale_fine
    for part, taps in ((total[3 * c1 : 9 * c1], 8), (last[3 * c1 :], 1)):
        turned = part.T * scale_coarse
        for ab in range(taps):
            for c in range(3):
                at = (8 if taps == 1 else ab) * 3 + c
                coarse[at] = turned[ab * c1 : (ab + 1) * c1, c * c2 : (c + 1) * c2]


def tree_sum(values):
    while len(values) > 1:
        values = [values[i] + values[i + 1] for i in range(0, len(values), 2)]
    return values[0]


def shapes(*pairs):
    return [pltpu.VMEM(shape, kind) for shape, kind in pairs]


def result(shape, kind):
    return jax.ShapeDtypeStruct(shape, kind)


def call(body, outs, args, flops=0, scratch=()):
    specs = [pl.BlockSpec(memory_space=pltpu.VMEM) for _ in args]
    nbytes = sum(a.size * a.dtype.itemsize for a in args)
    placed = [pltpu.with_memory_space_constraint(arg, pltpu.VMEM) for arg in args]
    return pl.pallas_call(
        body,
        out_shape=outs,
        in_specs=specs,
        out_specs=[pl.BlockSpec(memory_space=pltpu.VMEM) for _ in outs],
        scratch_shapes=list(scratch),
        compiler_params=pltpu.CompilerParams(vmem_limit_bytes=24 * 2**20),
        cost_estimate=pl.CostEstimate(flops=flops, bytes_accessed=nbytes, transcendentals=0),
    )(*placed)


def swap_pairs(even, odd, axis):
    nx, ny = lax.axis_size("gx"), lax.axis_size("gy")
    out = []
    for value, first in ((even, 0), (odd, 1)):
        pairs = []
        for place in range(nx * ny):
            at = [place // ny, place % ny]
            own = 0 if axis == "gx" else 1
            if first and at[own] in (0, (nx, ny)[own] - 1):
                at[1 - own] ^= 1
            else:
                at[own] = ((at[own] + first) ^ 1) - first
            pairs.append((place, at[0] * ny + at[1]))
        out.append(lax.ppermute(value, ("gx", "gy"), pairs))
    return out


def swap_bits(value, bits):
    ny = lax.axis_size("gy")
    count = lax.axis_size("gx") * ny
    flip = sum((bit if axis == "gy" else bit * ny) for axis, bit in bits)
    return lax.ppermute(value, ("gx", "gy"), [(i, i ^ flip) for i in range(count)])


def program(volume, fine_kernel, coarse_kernel, fine_cotangent, coarse_cotangent):
    c1, nz, ny, nx = volume.shape
    c2 = coarse_cotangent.shape[0]
    hz, hy, half = nz // 2, ny // 2, nx // 2
    gx, gy = lax.axis_size("gx"), lax.axis_size("gy")
    cells = nz * gx * ny * gy * nx
    sizes = dict(c1=c1, nz=nz, ny=ny, nx=nx)
    rows, half_rows = ny * c1, hy * c1

    own, z_even, z_odd = call(
        volume_rows_kernel,
        shapes(((rows, nz * nx), BF16), ((rows, nx), BF16), ((rows, nx), BF16)),
        [volume],
        flops=10**8,
    )
    z_even, z_odd = swap_pairs(z_even, z_odd, "gx")
    wa, wl, wh, wt, wc, wcl, wch, wct = call(
        functools.partial(weights_kernel, ny=ny),
        shapes(
            ((3 * ny * c1, 3 * ny * c1), BF16),
            ((3 * c1, 3 * c1), BF16),
            ((3 * c1, 3 * c1), BF16),
            ((3 * ny * c1, 3 * (ny + 2) * c1), BF16),
            ((3 * (hy + 2) * c2, 3 * hy * c1), BF16),
            ((6 * c2, 6 * c1), BF16),
            ((6 * c2, 6 * c1), BF16),
            ((3 * hy * c1, 3 * (hy + 2) * c2), BF16),
        ),
        [
            fine_kernel.reshape(27, c1, c1),
            coarse_kernel.swapaxes(3, 4).reshape(27, c1, c2),
        ],
        flops=10**9,
    )
    fine_cot, coarse_cot = call(
        cot_rows_kernel,
        shapes(((rows, nz * nx), BF16), ((hy * c2, hz * half), BF16)),
        [fine_cotangent, coarse_cotangent.reshape(c2, hz * hy, half)],
        flops=10**8,
    )

    layers = (nz + 2) * nx
    stacked = shapes(((rows, layers), BF16), ((c1, layers), BF16), ((c1, layers), BF16))
    own, y_even, y_odd = call(layers_kernel, stacked, [own, z_even, z_odd], flops=10**8)
    y_even, y_odd = swap_pairs(y_even, y_odd, "gy")

    pre, fine_rows, sums = call(
        functools.partial(fine_inner_kernel, c1=c1, nz=nz, nx=nx),
        shapes(
            ((rows, nz * nx), F32),
            ((rows - 2 * c1, nz * nx), BF16),
            ((rows - 2 * c1, hz * half), F32),
        ),
        [own, wa],
        flops=3 * 10**9,
    )
    sent = (half_rows, hz * half + 2 * half)
    pre_edge, fine_edge, pooled, z_even, z_odd = call(
        functools.partial(fine_edge_kernel, nz=nz, nx=nx),
        shapes(
            ((2 * c1, nz * nx), F32),
            ((2 * c1, nz * nx), BF16),
            ((half_rows, hz * half), BF16),
            (sent, BF16),
            (sent, BF16),
        ),
        [own, y_even, y_odd, wl, wh, pre, sums, coarse_cot],
        flops=10**9,
    )
    z_even, z_odd = swap_pairs(z_even, z_odd, "gx")
    fine_out, slopes, volume_rows = call(
        functools.partial(slope_kernel_fn, **sizes),
        [result((c1, nz, ny, nx), BF16)]
        + shapes(((rows, nz * nx), F32), ((rows + 2 * c1, layers), BF16)),
        [own, y_even, y_odd, pre, pre_edge, fine_rows, fine_edge],
        flops=2 * 10**9,
    )
    pooled_lanes = 3 * hz * half
    cot_lanes = (hz + 2) * half
    sent = (2 * c1, pooled_lanes + cot_lanes)
    pooled, coarse_cot, y_even, y_odd = call(
        coarse_layers_kernel,
        shapes(
            ((half_rows, pooled_lanes), BF16),
            ((hy * c2, cot_lanes), BF16),
            (sent, BF16),
            (sent, BF16),
        ),
        [pooled, coarse_cot, z_even, z_odd],
        flops=10**8,
    )
    y_even, y_odd = swap_pairs(y_even, y_odd, "gy")
    (pre,) = call(
        functools.partial(coarse_inner_kernel, count=hz + 2, half=half),
        shapes((((hy + 2) * c2, cot_lanes), F32)),
        [pooled, wc],
        flops=2 * 10**9,
    )

    pooled, coarse_slope, coarse_out, fslope, fgrad, z_even, z_odd = call(
        functools.partial(coarse_kernel_fn, c2=c2, **sizes),
        shapes(
            (((hy + 4) * c1, pooled_lanes), BF16),
            (((hy + 2) * c2, cot_lanes), BF16),
            ((c2 * hz * hy, half), BF16),
            ((rows, nz * nx), BF16),
            ((rows, nz * nx), F32),
            ((rows, nx), BF16),
            ((rows, nx), BF16),
        ),
        [pooled, coarse_cot, y_even, y_odd, fine_cot, slopes, pre, wcl, wch, wct],
        flops=4 * 10**9,
    )
    z_even, z_odd = swap_pairs(z_even, z_odd, "gx")
    (terms,) = call(
        functools.partial(terms_kernel, c1=c1, c2=c2, nx=nx),
        shapes(((11 * c1, 8 * c1), F32)),
        [volume_rows, fslope, pooled, coarse_slope],
        flops=2 * 10**9,
    )
    fslope, y_even, y_odd = call(layers_kernel, stacked, [fslope, z_even, z_odd], flops=10**8)
    y_even, y_odd = swap_pairs(y_even, y_odd, "gy")

    bits = [("gy", 1 << n) for n in range(gy.bit_length() - 1)]
    bits += [("gx", 1 << n) for n in range(gx.bit_length() - 1)]
    first = len(bits) % 2
    rounds = [bits[:1]] * first
    rounds += [bits[n : n + 2] for n in range(first, len(bits), 2)]
    value = terms
    for index, group in enumerate(rounds):
        if index:
            value = value.astype(BF16)
        parts = [value]
        for some in [[bit] for bit in group] + [group] * (len(group) == 2):
            parts.append(swap_bits(value, some))
        if index + 1 < len(rounds):
            value = tree_sum([part.astype(F32) for part in parts])
    volume_grad, coarse_out = call(
        functools.partial(volume_grad_kernel, **sizes),
        [result((c1, nz, ny, nx), BF16), result((c2 * hz * hy, half), BF16)],
        [fslope, y_even, y_odd, fgrad, wt, coarse_out],
        flops=2 * 10**9,
        scratch=[pltpu.VMEM((rows + 2 * c1, layers), BF16)],
    )
    fine_grad, coarse_grad = call(
        functools.partial(
            finish_kernel,
            c1=c1,
            c2=c2,
            scale_fine=cells ** (-0.5),
            scale_coarse=(cells // 8) ** (-0.5),
        ),
        [result((27, c1, c1), F32), result((27, c1, c2), F32)],
        parts,
        flops=10**7,
    )
    return (
        fine_out,
        coarse_out.reshape(c2, hz, hy, half),
        volume_grad,
        fine_grad.reshape(fine_kernel.shape),
        coarse_grad.reshape(3, 3, 3, c1, c2).swapaxes(3, 4),
    )


def solution(mesh):
    split = P(None, "gx", "gy", None)
    return jax.shard_map(
        program,
        mesh=mesh,
        in_specs=(split, P(), P(), split, split),
        out_specs=(split, split, split, P(), P()),
        check_vma=False,
    )
```

```python
import functools

import jax
import jax.numpy as jnp
from jax import lax
from jax.experimental import pallas as pl
from jax.experimental.pallas import tpu as pltpu
from jax.sharding import PartitionSpec as P


F32 = jnp.float32
BF16 = jnp.bfloat16


def mm(left, right):
    return jnp.dot(left, right, preferred_element_type=F32)


def mm_t(left, right):
    return lax.dot_general(left, right, (((1,), (1,)), ((), ())), preferred_element_type=F32)


def one_hot(shape, rule):
    rows = lax.broadcasted_iota(jnp.int32, shape, 0)
    cols = lax.broadcasted_iota(jnp.int32, shape, 1)
    return jnp.where(rule(rows, cols), 1.0, 0.0).astype(BF16)


def swap_matrix(outer, inner):
    count = outer * inner
    return one_hot((count, count), lambda r, c: c == (r % inner) * outer + r // inner)


def moved(values, width, offset):
    lanes = values.shape[1]
    place = lax.broadcasted_iota(jnp.int32, values.shape, 1) % width
    if offset == 1:
        return jnp.where(place == 0, 0.0, pltpu.roll(values, 1, 1))
    return jnp.where(place == width - 1, 0.0, pltpu.roll(values, lanes - 1, 1))


def combine(parts, width):
    rows = parts.shape[0] // 3
    return (
        parts[rows : 2 * rows]
        + moved(parts[:rows], width, 1)
        + moved(parts[2 * rows :], width, -1)
    )


def to_rows(values):
    chans, rows, width = values.shape
    return values.astype(F32).reshape(chans * rows, width).astype(BF16)


def band(taps_ref, out_ref, out_rows, in_rows, shift, turned, flipped):
    m, n = taps_ref.shape[1:][::-1] if turned else taps_ref.shape[1:]
    wide = in_rows * n
    spread = one_hot((n, wide), lambda r, c: c % n == r)
    block = lax.broadcasted_iota(jnp.int32, (m, wide), 1) // n
    if turned:
        tiled = [
            lax.dot_general(
                taps_ref[at], spread, (((0,), (0,)), ((), ())), preferred_element_type=F32
            )
            for at in range(27)
        ]
    else:
        every = mm(taps_ref[...].reshape(27 * m, n), spread)
        tiled = [every[at * m : (at + 1) * m] for at in range(27)]
    if flipped:
        tiled = tiled[::-1]
    for a in range(3):
        for c in range(3):
            taps = [tiled[(a * 3 + b) * 3 + c] for b in range(3)]
            for y in range(out_rows):
                value = jnp.zeros((m, wide), F32)
                for b in range(3):
                    if 0 <= y + b - shift < in_rows:
                        value = jnp.where(block == y + b - shift, taps[b], value)
                start = (c * out_rows + y) * m
                out_ref[start : start + m, a * wide : (a + 1) * wide] = value.astype(BF16)


def weights_kernel(kf, kc, wa, wl, wh, wt, wc, wcl, wch, wct, *, ny):
    hy = ny // 2
    band(kf, wa, ny, ny, 1, False, False)
    band(kf, wl, 1, 1, 0, False, False)
    band(kf, wh, 1, 1, 2, False, False)
    band(kc, wc, hy + 2, hy, 2, True, False)
    band(kc, wcl, 2, 2, 0, True, False)
    band(kc, wch, 2, 2, 2, True, False)
    band(kf, wt, ny, ny + 2, 0, True, True)
    band(kc, wct, hy, hy + 2, 0, False, True)


def ends():
    return [lax.axis_index(axis) % 2 == 0 for axis in ("gx", "gy")]


def from_odd(value, axis):
    at = lax.axis_index(axis)
    alone = jnp.logical_or(at == 0, at == lax.axis_size(axis) - 1)
    return jnp.where(alone, jnp.zeros_like(value), value)


def volume_rows_kernel(vol, own, even, odd):
    c1, nz, ny, nx = vol.shape
    swap = swap_matrix(ny, c1)
    for z in range(nz):
        own[:, z * nx : (z + 1) * nx] = mm(swap, to_rows(vol[:, z])).astype(BF16)
    low, high = own[:, : even.shape[1]], own[:, own.shape[1] - even.shape[1] :]
    first = ends()[0]
    even[...] = jnp.where(first, high, low)
    odd[...] = jnp.where(first, low, high)


def cot_rows_kernel(fc, cc, fine, coarse):
    c1, nz, ny, nx = fc.shape
    c2, cells, half = cc.shape
    hy = ny // 2
    swap = swap_matrix(ny, c1)
    for z in range(nz):
        fine[:, z * nx : (z + 1) * nx] = mm(swap, to_rows(fc[:, z])).astype(BF16)
    rows = mm(swap_matrix(cells, c2), to_rows(cc[...])).astype(BF16)
    for z in range(cells // hy):
        coarse[:, z * half : (z + 1) * half] = rows[z * hy * c2 : (z + 1) * hy * c2]


def stack_layers(out, own, even, odd):
    first = ends()[0]
    width = even.shape[1]
    low, high = even[...], from_odd(odd[...], "gx")
    out[:, :width] = jnp.where(first, high, low)
    out[:, width : width + own.shape[1]] = own[...]
    out[:, width + own.shape[1] :] = jnp.where(first, low, high)


def stack_rows(out, own, even, odd):
    first = ends()[1]
    edge = even.shape[0]
    low, high = even[...], from_odd(odd[...], "gy")
    out[:edge] = jnp.where(first, high, low)
    out[edge : edge + own.shape[0]] = own[...]
    out[edge + own.shape[0] :] = jnp.where(first, low, high)


def layers_kernel(own, z_even, z_odd, out, even, odd):
    stack_layers(out, own, z_even, z_odd)
    edge = even.shape[0]
    first = ends()[1]
    low, high = out[:edge], out[out.shape[0] - edge :]
    even[...] = jnp.where(first, high, low)
    odd[...] = jnp.where(first, low, high)


def coarse_layers_kernel(po, co, z_even, z_odd, p_out, c_out, even, odd):
    lanes, rows = po.shape[1], po.shape[0]
    half = (z_even.shape[1] - lanes) // 2
    stack_layers(p_out, po, z_even.at[:, :lanes], z_odd.at[:, :lanes])
    first = ends()[0]
    width = co.shape[1]
    for part in range(2):
        span = slice(lanes + part * half, lanes + (part + 1) * half)
        low, high = z_even[:, span], from_odd(z_odd[:, span], "gx")
        into = slice(part * rows, (part + 1) * rows)
        c_out[into, :half] = jnp.where(first, high, low)
        c_out[into, half + width :] = jnp.where(first, low, high)
    c_out[:, half : half + width] = co[...]
    edge = even.shape[0]
    pooled = p_out.shape[1]
    first = ends()[1]
    for ref, span in ((p_out, slice(0, pooled)), (c_out, slice(pooled, even.shape[1]))):
        low, high = ref[:edge], ref[ref.shape[0] - edge :]
        even[:, span] = jnp.where(first, high, low)
        odd[:, span] = jnp.where(first, low, high)


def three_layers(ref, rows, first, step, width):
    return jnp.concatenate(
        [ref[rows, first + dz * step : first + dz * step + width] for dz in range(3)], axis=0
    )


def neighbours(even, odd, axis):
    first = ends()[0 if axis == "gx" else 1]
    odd = from_odd(odd, axis)
    return jnp.where(first, odd, even), jnp.where(first, even, odd)


def all_layers(values, count, step):
    return jnp.concatenate([values[:, dz * step : (dz + count) * step] for dz in range(3)], axis=0)


def fine_inner_kernel(xo, wa, pre_out, fo_out, sums_out, *, c1, nz, nx):
    half = nx // 2
    pool = one_hot((nx, half), lambda r, c: r // 2 == c)
    inner = slice(c1, xo.shape[0] - c1)
    for layer in range(nz):
        pre = combine(mm(wa[...], three_layers(xo, slice(None), layer * nx, nx, nx)), nx)
        span = slice(layer * nx, (layer + 1) * nx)
        pre_out[:, span] = pre
        pre = pre[inner]
        value = xo[inner, (layer + 1) * nx : (layer + 2) * nx].astype(F32)
        fo = (value + pre * jax.nn.sigmoid(pre)).astype(BF16)
        fo_out[:, span] = fo
        pooled = mm(fo, pool)
        sums = pooled if layer % 2 == 0 else sums + pooled
        if layer % 2:
            sums_out[:, layer // 2 * half : (layer // 2 + 1) * half] = sums


def fine_edge_kernel(
    xo, y_even, y_odd, wl, wh, pre_ref, sums, co, pre_out, fo_out, po, z_even, z_odd, *, nz, nx
):
    c1 = y_even.shape[0]
    half = nx // 2
    rows = xo.shape[0]
    low, high = neighbours(y_even[...], y_odd[...], "gy")
    last = slice(rows - c1, rows)
    pre = jnp.concatenate(
        [
            pre_ref[:c1] + combine(mm(wl[...], all_layers(low, nz, nx)), nx),
            pre_ref[last] + combine(mm(wh[...], all_layers(high, nz, nx)), nx),
        ],
        axis=0,
    )
    pre_out[...] = pre
    own = slice(nx, (nz + 1) * nx)
    value = jnp.concatenate([xo[:c1, own], xo[last, own]], axis=0).astype(F32)
    fo = (value + pre * jax.nn.sigmoid(pre)).astype(BF16)
    fo_out[...] = fo
    pool = one_hot((nx, half), lambda r, c: r // 2 == c)
    for place in range(nz // 2):
        first = 2 * place * nx
        pooled = mm(fo[:, first : first + nx], pool) + mm(fo[:, first + nx : first + 2 * nx], pool)
        span = slice(place * half, (place + 1) * half)
        cells = [pooled[:c1]] + [sums[r * c1 : (r + 1) * c1, span] for r in range(rows // c1 - 2)]
        cells.append(pooled[c1:])
        cells = [cells[r] + cells[r + 1] for r in range(0, len(cells), 2)]
        po[:, span] = (jnp.concatenate(cells, axis=0) * 0.125).astype(BF16)
    lanes = po.shape[1]
    low, high = co[:, :half], co[:, co.shape[1] - half :]
    first = ends()[0]
    for ref, value in (
        (z_even, jnp.where(first, high, low)),
        (z_odd, jnp.where(first, low, high)),
    ):
        ref[:, :lanes] = po[...]
        ref[:, lanes : lanes + half] = value[: rows // 2]
        ref[:, lanes + half :] = value[rows // 2 :]


def slope_kernel_fn(
    xo, y_even, y_odd, pre_ref, pre_edge, fo, fo_edge, fo_out, sl_out, x_ref, *, c1, nz, ny, nx
):
    stack_rows(x_ref, xo, y_even, y_odd)
    swap_back = swap_matrix(c1, ny)
    for layer in range(nz):
        span = slice(layer * nx, (layer + 1) * nx)
        pre = jnp.concatenate(
            [pre_edge[:c1, span], pre_ref[c1 : c1 * (ny - 1), span], pre_edge[c1:, span]], axis=0
        )
        sig = jax.nn.sigmoid(pre)
        sl_out[:, span] = sig * (1.0 + pre * (1.0 - sig))
        rows = jnp.concatenate([fo_edge[:c1, span], fo[:, span], fo_edge[c1:, span]], axis=0)
        fo_out[:, layer] = mm(swap_back, rows).reshape(c1, ny, nx).astype(BF16)


def coarse_inner_kernel(po, wc, pre_out, *, count, half):
    for pair in range(count // 2):
        parts = mm(wc[...], three_layers(po, slice(None), pair * 2 * half, half, 2 * half))
        pre_out[:, pair * 2 * half : (pair + 1) * 2 * half] = combine(parts, half)


def coarse_kernel_fn(
    po, cc, y_even, y_odd, fc, sl, pre_ref, wcl, wch, wct,
    p_ref, cs_ref, co_out, fs_out, fg_out, z_even, z_odd, *, c1, c2, nz, ny, nx,
):
    half, hz, hy = nx // 2, nz // 2, ny // 2
    pooled = po.shape[1]
    low, high = neighbours(y_even[...], y_odd[...], "gy")
    edge = low.shape[0]
    p_ref[:edge] = low[:, :pooled]
    p_ref[edge : edge + po.shape[0]] = po[...]
    p_ref[edge + po.shape[0] :] = high[:, :pooled]
    count = hz + 2
    pre = jnp.concatenate(
        [
            combine(mm(wcl[...], all_layers(low[:, :pooled], count, half)), half),
            jnp.zeros(((hy - 2) * c2, count * half), F32),
            combine(mm(wch[...], all_layers(high[:, :pooled], count, half)), half),
        ],
        axis=0,
    )
    pre = pre + pre_ref[...]
    sig = jax.nn.sigmoid(pre)
    cot = jnp.concatenate([low[:, pooled:], cc[...], high[:, pooled:]], axis=0).astype(F32)
    cs_ref[...] = (cot * (sig * (1.0 + pre * (1.0 - sig)))).astype(BF16)
    inner = slice(c2, c2 + hy * c2)
    out = (pre[inner, half:-half] * sig[inner, half:-half]).astype(BF16)
    stacked = jnp.concatenate([out[:, z * half : (z + 1) * half] for z in range(hz)], axis=0)
    co_out[...] = mm(swap_matrix(c2, hz * hy), stacked).astype(BF16)
    widen = one_hot((half, nx), lambda r, c: c // 2 == r)
    for pair in range(hz // 2):
        parts = mm(wct[...], three_layers(cs_ref, slice(None), pair * nx, half, nx))
        grad = combine(parts, half) * 0.125
        high = grad.astype(BF16)
        low = (grad - high.astype(F32)).astype(BF16)
        for side in range(2):
            lanes = slice(side * half, (side + 1) * half)
            up = mm(high[:, lanes], widen) + mm(low[:, lanes], widen)
            blocks = [up[y // 2 * c1 : y // 2 * c1 + c1] for y in range(ny)]
            spread = jnp.concatenate(blocks, axis=0)
            for layer in (4 * pair + 2 * side, 4 * pair + 2 * side + 1):
                span = slice(layer * nx, (layer + 1) * nx)
                total = fc[:, span].astype(F32) + spread
                fg_out[:, span] = total
                fs_out[:, span] = (total * sl[:, span]).astype(BF16)
    low, high = fs_out[:, :nx], fs_out[:, (nz - 1) * nx :]
    first = ends()[0]
    z_even[...] = jnp.where(first, high, low)
    z_odd[...] = jnp.where(first, low, high)


def terms_of(slopes, cells, chans, count, width, rows, lanes):
    slopes = slopes.astype(F32)
    shifted = [moved(slopes, width, -1), slopes, moved(slopes, width, 1)]
    shifted = [value.astype(BF16) for value in shifted]
    total = None
    for y in range(slopes.shape[0] // chans):
        left = jnp.concatenate([s[y * chans : (y + 1) * chans] for s in shifted], axis=0)
        first = y * count + rows
        right = [
            cells[first : first + 3 * count, lanes + a * width : lanes + a * width + slopes.shape[1]]
            for a in range(3)
        ]
        term = mm_t(left, jnp.concatenate(right, axis=0))
        total = term if total is None else total + term
    return total


def terms_kernel(x_ref, fs, p_ref, cs, g_out, *, c1, c2, nx):
    half = nx // 2
    fine = terms_of(fs[...], x_ref, c1, c1, nx, 0, 0)
    inner = cs[c2 : cs.shape[0] - c2, half : cs.shape[1] - half]
    coarse = terms_of(inner, p_ref, c2, c1, half, c1, half)
    three = 3 * c1
    g_out[:three, :] = fine[:, : 8 * c1]
    g_out[three : 9 * c1, :] = coarse[:, : 8 * c1]
    last = jnp.concatenate([fine[:, 8 * c1 :], coarse[:, 8 * c1 :]], axis=0)
    groups = [last[r * c1 : (r + 1) * c1] for r in range(9)]
    g_out[9 * c1 : 10 * c1, :] = jnp.concatenate(groups[:8], axis=1)
    g_out[10 * c1 :, :] = jnp.concatenate([groups[8]] * 8, axis=1)


def volume_grad_kernel(fs, y_even, y_odd, fg, wt, co, out, co_out, rows_ref, *, c1, nz, ny, nx):
    swap_back = swap_matrix(c1, ny)
    stack_rows(rows_ref, fs, y_even, y_odd)
    for layer in range(nz):
        parts = mm(wt[...], three_layers(rows_ref, slice(None), layer * nx, nx, nx))
        total = fg[:, layer * nx : (layer + 1) * nx] + combine(parts, nx)
        out[:, layer] = mm(swap_back, total.astype(BF16)).reshape(c1, ny, nx).astype(BF16)
    co_out[...] = co[...]


def finish_kernel(*refs, c1, c2, scale_fine, scale_coarse):
    parts, (fine, coarse) = refs[:-2], refs[-2:]
    total = tree_sum([part[...].astype(F32) for part in parts])
    tail = total[9 * c1 :]
    groups = [tail[:c1, r * c1 : (r + 1) * c1] for r in range(8)] + [tail[c1:, :c1]]
    last = jnp.concatenate(groups, axis=0)
    for c in range(3):
        own = slice(c * c1, (c + 1) * c1)
        for ab in range(8):
            fine[ab * 3 + c] = total[own, ab * c1 : (ab + 1) * c1] * scale_fine
        fine[24 + c] = last[own] * scale_fine
    for part, taps in ((total[3 * c1 : 9 * c1], 8), (last[3 * c1 :], 1)):
        turned = part.T * scale_coarse
        for ab in range(taps):
            for c in range(3):
                at = (8 if taps == 1 else ab) * 3 + c
                coarse[at] = turned[ab * c1 : (ab + 1) * c1, c * c2 : (c + 1) * c2]


def tree_sum(values):
    while len(values) > 1:
        values = [values[i] + values[i + 1] for i in range(0, len(values), 2)]
    return values[0]


def shapes(*pairs):
    return [pltpu.VMEM(shape, kind) for shape, kind in pairs]


def result(shape, kind):
    return jax.ShapeDtypeStruct(shape, kind)


def call(body, outs, args, flops=0, scratch=()):
    specs = [pl.BlockSpec(memory_space=pltpu.VMEM) for _ in args]
    nbytes = sum(a.size * a.dtype.itemsize for a in args)
    placed = [pltpu.with_memory_space_constraint(arg, pltpu.VMEM) for arg in args]
    return pl.pallas_call(
        body,
        out_shape=outs,
        in_specs=specs,
        out_specs=[pl.BlockSpec(memory_space=pltpu.VMEM) for _ in outs],
        scratch_shapes=list(scratch),
        compiler_params=pltpu.CompilerParams(vmem_limit_bytes=24 * 2**20),
        cost_estimate=pl.CostEstimate(flops=flops, bytes_accessed=nbytes, transcendentals=0),
    )(*placed)


def swap_pairs(even, odd, axis):
    nx, ny = lax.axis_size("gx"), lax.axis_size("gy")
    out = []
    for value, first in ((even, 0), (odd, 1)):
        pairs = []
        for place in range(nx * ny):
            at = [place // ny, place % ny]
            own = 0 if axis == "gx" else 1
            if first and at[own] in (0, (nx, ny)[own] - 1):
                at[1 - own] ^= 1
            else:
                at[own] = ((at[own] + first) ^ 1) - first
            pairs.append((place, at[0] * ny + at[1]))
        out.append(lax.ppermute(value, ("gx", "gy"), pairs))
    return out


def swap_bits(value, bits, odd_bits=()):
    ny = lax.axis_size("gy")
    count = lax.axis_size("gx") * ny
    flip, more = (
        sum((bit if axis == "gy" else bit * ny) for axis, bit in some) for some in (bits, odd_bits)
    )
    return lax.ppermute(
        value, ("gx", "gy"), [(i, i ^ flip ^ (more if i % 2 else 0)) for i in range(count)]
    )


def program(volume, fine_kernel, coarse_kernel, fine_cotangent, coarse_cotangent):
    c1, nz, ny, nx = volume.shape
    c2 = coarse_cotangent.shape[0]
    hz, hy, half = nz // 2, ny // 2, nx // 2
    gx, gy = lax.axis_size("gx"), lax.axis_size("gy")
    cells = nz * gx * ny * gy * nx
    sizes = dict(c1=c1, nz=nz, ny=ny, nx=nx)
    rows, half_rows = ny * c1, hy * c1

    own, z_even, z_odd = call(
        volume_rows_kernel,
        shapes(((rows, nz * nx), BF16), ((rows, nx), BF16), ((rows, nx), BF16)),
        [volume],
        flops=10**8,
    )
    z_even, z_odd = swap_pairs(z_even, z_odd, "gx")
    wa, wl, wh, wt, wc, wcl, wch, wct = call(
        functools.partial(weights_kernel, ny=ny),
        shapes(
            ((3 * ny * c1, 3 * ny * c1), BF16),
            ((3 * c1, 3 * c1), BF16),
            ((3 * c1, 3 * c1), BF16),
            ((3 * ny * c1, 3 * (ny + 2) * c1), BF16),
            ((3 * (hy + 2) * c2, 3 * hy * c1), BF16),
            ((6 * c2, 6 * c1), BF16),
            ((6 * c2, 6 * c1), BF16),
            ((3 * hy * c1, 3 * (hy + 2) * c2), BF16),
        ),
        [
            fine_kernel.reshape(27, c1, c1),
            coarse_kernel.swapaxes(3, 4).reshape(27, c1, c2),
        ],
        flops=10**9,
    )
    fine_cot, coarse_cot = call(
        cot_rows_kernel,
        shapes(((rows, nz * nx), BF16), ((hy * c2, hz * half), BF16)),
        [fine_cotangent, coarse_cotangent.reshape(c2, hz * hy, half)],
        flops=10**8,
    )

    layers = (nz + 2) * nx
    stacked = shapes(((rows, layers), BF16), ((c1, layers), BF16), ((c1, layers), BF16))
    own, y_even, y_odd = call(layers_kernel, stacked, [own, z_even, z_odd], flops=10**8)
    y_even, y_odd = swap_pairs(y_even, y_odd, "gy")

    pre, fine_rows, sums = call(
        functools.partial(fine_inner_kernel, c1=c1, nz=nz, nx=nx),
        shapes(
            ((rows, nz * nx), F32),
            ((rows - 2 * c1, nz * nx), BF16),
            ((rows - 2 * c1, hz * half), F32),
        ),
        [own, wa],
        flops=3 * 10**9,
    )
    sent = (half_rows, hz * half + 2 * half)
    pre_edge, fine_edge, pooled, z_even, z_odd = call(
        functools.partial(fine_edge_kernel, nz=nz, nx=nx),
        shapes(
            ((2 * c1, nz * nx), F32),
            ((2 * c1, nz * nx), BF16),
            ((half_rows, hz * half), BF16),
            (sent, BF16),
            (sent, BF16),
        ),
        [own, y_even, y_odd, wl, wh, pre, sums, coarse_cot],
        flops=10**9,
    )
    z_even, z_odd = swap_pairs(z_even, z_odd, "gx")
    fine_out, slopes, volume_rows = call(
        functools.partial(slope_kernel_fn, **sizes),
        [result((c1, nz, ny, nx), BF16)]
        + shapes(((rows, nz * nx), F32), ((rows + 2 * c1, layers), BF16)),
        [own, y_even, y_odd, pre, pre_edge, fine_rows, fine_edge],
        flops=2 * 10**9,
    )
    pooled_lanes = 3 * hz * half
    cot_lanes = (hz + 2) * half
    sent = (2 * c1, pooled_lanes + cot_lanes)
    pooled, coarse_cot, y_even, y_odd = call(
        coarse_layers_kernel,
        shapes(
            ((half_rows, pooled_lanes), BF16),
            ((hy * c2, cot_lanes), BF16),
            (sent, BF16),
            (sent, BF16),
        ),
        [pooled, coarse_cot, z_even, z_odd],
        flops=10**8,
    )
    y_even, y_odd = swap_pairs(y_even, y_odd, "gy")
    (pre,) = call(
        functools.partial(coarse_inner_kernel, count=hz + 2, half=half),
        shapes((((hy + 2) * c2, cot_lanes), F32)),
        [pooled, wc],
        flops=2 * 10**9,
    )

    pooled, coarse_slope, coarse_out, fslope, fgrad, z_even, z_odd = call(
        functools.partial(coarse_kernel_fn, c2=c2, **sizes),
        shapes(
            (((hy + 4) * c1, pooled_lanes), BF16),
            (((hy + 2) * c2, cot_lanes), BF16),
            ((c2 * hz * hy, half), BF16),
            ((rows, nz * nx), BF16),
            ((rows, nz * nx), F32),
            ((rows, nx), BF16),
            ((rows, nx), BF16),
        ),
        [pooled, coarse_cot, y_even, y_odd, fine_cot, slopes, pre, wcl, wch, wct],
        flops=4 * 10**9,
    )
    z_even, z_odd = swap_pairs(z_even, z_odd, "gx")
    (terms,) = call(
        functools.partial(terms_kernel, c1=c1, c2=c2, nx=nx),
        shapes(((11 * c1, 8 * c1), F32)),
        [volume_rows, fslope, pooled, coarse_slope],
        flops=2 * 10**9,
    )
    fslope, y_even, y_odd = call(layers_kernel, stacked, [fslope, z_even, z_odd], flops=10**8)
    y_even, y_odd = swap_pairs(y_even, y_odd, "gy")

    bits = [("gy", 1 << n) for n in range(gy.bit_length() - 1)]
    bits += [("gx", 1 << n) for n in range(gx.bit_length() - 1)]
    first = len(bits) % 2
    rounds = [bits[:1]] * first
    rounds += [bits[n : n + 2] for n in range(first, len(bits), 2)]
    value = terms
    for index, group in enumerate(rounds):
        if index:
            value = value.astype(BF16)
        parts = [value, swap_bits(value, group[:1])]
        if len(group) == 2:
            fetched = swap_bits(value, group[1:], group[:1])
            parts += [fetched, swap_bits(fetched, bits[:1])]
        if index + 1 < len(rounds):
            value = tree_sum([part.astype(F32) for part in parts])
    volume_grad, coarse_out = call(
        functools.partial(volume_grad_kernel, **sizes),
        [result((c1, nz, ny, nx), BF16), result((c2 * hz * hy, half), BF16)],
        [fslope, y_even, y_odd, fgrad, wt, coarse_out],
        flops=2 * 10**9,
        scratch=[pltpu.VMEM((rows + 2 * c1, layers), BF16)],
    )
    fine_grad, coarse_grad = call(
        functools.partial(
            finish_kernel,
            c1=c1,
            c2=c2,
            scale_fine=cells ** (-0.5),
            scale_coarse=(cells // 8) ** (-0.5),
        ),
        [result((27, c1, c1), F32), result((27, c1, c2), F32)],
        parts,
        flops=10**7,
    )
    return (
        fine_out,
        coarse_out.reshape(c2, hz, hy, half),
        volume_grad,
        fine_grad.reshape(fine_kernel.shape),
        coarse_grad.reshape(3, 3, 3, c1, c2).swapaxes(3, 4),
    )


def solution(mesh):
    split = P(None, "gx", "gy", None)
    return jax.shard_map(
        program,
        mesh=mesh,
        in_specs=(split, P(), P(), split, split),
        out_specs=(split, split, split, P(), P()),
        check_vma=False,
    )
```
